256 devices in a mesh: seq: 32 (over z, x_hi, core), exp: 8 (over x_lo, y).
Axes of the slice: x: 4 (x_hi: 2, x_lo: 2; x = x_hi * 2 + x_lo), y: 4, z: 8, core: 2. Of those that a mesh axis runs over, the one named last changes fastest.
Arguments:
- queries: bfloat16 [3072, 4096], P('seq', 'exp'), may hold values from -17 to 17
- keys: bfloat16 [3072, 1024], P('seq', 'exp'), may hold values from -17 to 17
- values: bfloat16 [3072, 1024], P('seq', 'exp'), may hold values from -6 to 6
- residual: bfloat16 [3072, 4096], P('seq', 'exp'), may hold values from -48 to 48
- norm_gain: float32 [4096], P('exp'), may hold values from 0.1 to 1.9
- routes: int32 [3072, 2], P('seq'), may hold values from 0 to 7, all different within a row; in each aligned block of 96 rows (0 to 95, 96 to 191, ...) at most 36 rows name the same one
- gates: float32 [3072, 2], P('seq'), may hold values from 0.1 to 0.9
- w_gate: bfloat16 [8, 4096, 14336], P('exp', None, 'seq'), may hold values from -0.09375 to 0.09375
- w_up: bfloat16 [8, 4096, 14336], P('exp', None, 'seq'), may hold values from -0.09375 to 0.09375
- w_down: bfloat16 [8, 14336, 4096], P('exp', 'seq'), may hold values from -0.046875 to 0.046875
Outputs:
- attended: bfloat16 [3072, 4096], P('seq', 'exp')
- layer_out: bfloat16 [3072, 4096], P('seq', 'exp')
The draws below stay inside these ranges and needn't reach their ends.
Inputs may be any that keep to these rules, and one draw needn't show every extreme that they name: `routes`: each row names 2 different experts. In the rows of one device no expert is named more than 36 times, a bound that some block reaches.
All inputs are finite; a program needn't handle non-finite values.
Results may differ from the reference program's by a relative error of at most 0.0075.
Values may be sent and summed in bfloat16 or wider, within the bound.
A program may use at most 128 MiB of HBM per device.

```python
import math
import jax
import jax.numpy as jnp
import numpy as np
from jax import lax

D = 4096
QUERY_HEADS = 32
KEY_VALUE_HEADS = 8
HEAD_WIDTH = 128
FF = 14336
TOP = 2
TOK_DEV = 96
SEQUENCE_LENGTH = 3072
EXPERTS = 8
CAP = 36
N_SEQ = 32


def draw_keys(key, part):
    layer_result = jnp.clip(jax.random.normal(jax.random.fold_in(key, 2), (SEQUENCE_LENGTH, KEY_VALUE_HEADS * HEAD_WIDTH), jnp.float32), -4.0, 4.0)
    layer_result = jnp.clip(layer_result, -16.5, 16.5)
    return layer_result.astype(jnp.bfloat16)


def draw_queries(key, part):
    layer_result = jnp.clip(jax.random.normal(jax.random.fold_in(key, 1), (SEQUENCE_LENGTH, QUERY_HEADS * HEAD_WIDTH), jnp.float32), -4.0, 4.0)
    layer_result = jnp.clip(layer_result, -16.5, 16.5)
    return layer_result.astype(jnp.bfloat16)


def draw_residual(key, part):
    base = jnp.clip(jax.random.normal(jax.random.fold_in(key, 5), (SEQUENCE_LENGTH, D), jnp.float32), -4.0, 4.0)
    column = jnp.arange(D, dtype=jnp.float32) / max(D - 1, 1)
    column_scale = 0.6 * jnp.exp(column * math.log(5.0))
    layer_result = base * column_scale[None, :]
    return layer_result.astype(jnp.bfloat16)


def steps_of(key, extent, shards, smallest, top_value):
    loudness = 1.0
    for axis_at, shards_of in shards:
        steps = jax.random.uniform(jax.random.fold_in(jax.random.fold_in(key, 6), axis_at), (shards_of,), jnp.float32, smallest / len(shards), top_value / len(shards))
        loudness = loudness * jnp.repeat(jnp.exp(steps), extent[axis_at] // shards_of).reshape((-1,) + (1,) * (len(extent) - 1 - axis_at))
    return loudness


def assign_block(key, own, number, rows, amount, top, bound, skew):
    ranking = jax.random.permutation(key, amount)
    packed, common = shares(amount, rows * top, bound, skew, True), shares(amount, rows * top, bound, skew, False)
    places = jnp.arange(amount)

    def named(tallies, offset_by):
        used = int((tallies > 0).sum())
        fixed = max(1, used // 4)
        moved = fixed + (places - fixed + offset_by * (used - fixed)) % max(1, amount - fixed)
        return jnp.zeros((amount,), jnp.int32).at[ranking[jnp.where(places < fixed, places, moved)]].set(jnp.asarray(tallies, jnp.int32))

    tallies = jnp.where(number % 4 == 0, named(packed, number // 4), named(common, number - number // 4 - 1))
    mixed = jax.random.permutation(jax.random.fold_in(own, 3), amount)
    source_of, taker = mixed[0:amount // 2 * 2:2], mixed[1:amount // 2 * 2:2]
    room = jnp.minimum(tallies[source_of] - 1, bound - tallies[taker]) // 2
    room = jnp.where((source_of == ranking[0]) | (taker == ranking[0]) | (tallies[taker] == 0), 0, jnp.maximum(room, 0))
    moved = jax.random.randint(jax.random.fold_in(own, 4), (amount // 2,), 0, 1 << 20) % (room + 1)
    tallies = tallies.at[source_of].add(-moved).at[taker].add(moved)
    labels = jnp.searchsorted(jnp.cumsum(tallies), jnp.arange(rows * top), side="right").astype(jnp.int32)
    grid = labels.reshape(top, rows).T
    grid = grid[jax.random.permutation(jax.random.fold_in(own, 1), rows)]
    offset_by = jax.random.randint(jax.random.fold_in(own, 2), (rows, 1), 0, top)
    return jnp.take_along_axis(grid, (jnp.arange(top)[None, :] + offset_by) % top, axis=1)


def shares(number_of, total, limit, lean, full):
    loads = [(1 << 20) // math.isqrt(rank ** lean) + 1 for rank in range(1, number_of + 1)]
    largest = limit if full else min(limit, max(-(-total // number_of), total * loads[0] // sum(loads)))
    least = 1 if total - largest >= number_of - 1 else 0
    given, rest = [largest] + [least] * (number_of - 1), total - largest - least * (number_of - 1)
    while rest > 0:
        free = [i for i in range(1, number_of) if given[i] < largest] or [i for i in range(1, number_of) if given[i] < limit]
        pool, left = sum([loads[i] for i in free]), rest
        for i in free:
            more = min(limit - given[i], max(1, left * loads[i] // pool), rest)
            given[i] = given[i] + more
            rest = rest - more
    return np.array(given)


def noise(stream_key, extent, deviation, limit, split=(), kind=jnp.bfloat16):
    result = deviation * jax.random.normal(stream_key, extent, jnp.float32)
    if split:
        result = result * steps_of(stream_key, extent, split, -0.22, 0.18)
    return jnp.clip(result, -limit, limit).astype(kind)


def setup_inputs(seed: int = 0) -> dict:
    seeds = jax.random.split(jax.random.key(seed), 11)
    queries = draw_queries(jax.random.fold_in(seeds[10], 71), 0)
    keys = draw_keys(jax.random.fold_in(seeds[10], 71), 0)
    values = noise(seeds[2], (SEQUENCE_LENGTH, KEY_VALUE_HEADS * HEAD_WIDTH), 1.0, 6.0, ((0, 32), (1, 8)))
    residual = draw_residual(jax.random.fold_in(seeds[10], 71), 0)
    norm_gain = jnp.clip(1.0 + 0.18 * jax.random.normal(seeds[4], (D,), jnp.float32), 0.1, 1.9)
    routes_keys = jax.random.split(jax.random.fold_in(seeds[5], 1), SEQUENCE_LENGTH // TOK_DEV)
    routes_turns = jax.random.permutation(jax.random.fold_in(seeds[5], 3), SEQUENCE_LENGTH // TOK_DEV)
    routes = jax.vmap(lambda own, number: assign_block(jax.random.fold_in(seeds[5], 2), own, number, TOK_DEV, EXPERTS, TOP, CAP, 2))(routes_keys, routes_turns).reshape((SEQUENCE_LENGTH, TOP))
    gates = jnp.clip(0.1 + 0.79999997 * jax.random.uniform(seeds[6], (SEQUENCE_LENGTH, TOP), jnp.float32) ** steps_of(seeds[6], (SEQUENCE_LENGTH, TOP), ((0, 32),), -0.2, 0.2), 0.1, 0.9)
    w_gate = noise(seeds[7], (EXPERTS, D, FF), D ** -0.5, 0.09375, ((0, 8), (2, 32)))
    w_up = noise(seeds[8], (EXPERTS, D, FF), D ** -0.5, 0.09375, ((0, 8), (2, 32)))
    w_down = noise(seeds[9], (EXPERTS, FF, D), FF ** -0.5, 0.046875, ((0, 8), (1, 32)))
    return {"queries": queries, "keys": keys, "values": values, "residual": residual, "norm_gain": norm_gain, "routes": routes, "gates": gates, "w_gate": w_gate, "w_up": w_up, "w_down": w_down}


def attend_head(inputs):
    query_head, key_head, value_head = inputs
    scores = jnp.einsum('tgd,pd->gtp', query_head, key_head) / math.sqrt(HEAD_WIDTH)
    positions = jnp.arange(SEQUENCE_LENGTH, dtype=jnp.int32)
    causal_mask = (positions[None, :] <= positions[:, None])[None, :, :]
    scores = jnp.where(causal_mask, scores, -1e+30)
    row_max = lax.optimization_barrier(jnp.max(scores, axis=-1, keepdims=True))
    exp_terms = jnp.where(causal_mask, jnp.exp(scores - row_max), 0.0)
    denominator = lax.optimization_barrier(jnp.sum(exp_terms, axis=-1))
    probs_low = exp_terms.astype(jnp.bfloat16).astype(jnp.float32)
    return jnp.einsum('gtp,pd->gtd', probs_low, value_head) / denominator[..., None]

def expert_apply(inputs):
    rows, gate_mat, up_mat, down_mat = inputs
    hidden = (jax.nn.silu(jnp.dot(rows, gate_mat, preferred_element_type=jnp.float32)) * jnp.dot(rows, up_mat, preferred_element_type=jnp.float32)).astype(jnp.bfloat16)
    row_count = rows.shape[0]
    block_width = FF // N_SEQ
    hidden_blocks = jnp.transpose(hidden.reshape(row_count, N_SEQ, block_width), (1, 0, 2))
    down_blocks = down_mat.reshape(N_SEQ, block_width, D)

    def add_block(total, pair):
        hidden_block, down_block = pair
        term = jnp.dot(hidden_block, down_block, preferred_element_type=jnp.float32).astype(jnp.bfloat16)
        term = lax.optimization_barrier(term)
        return (total + term.astype(jnp.float32), None)
    total, unused = lax.scan(add_block, jnp.zeros((row_count, D), jnp.float32), (hidden_blocks, down_blocks))
    return total.astype(jnp.bfloat16)

def reference(queries, keys, values, residual, norm_gain, routes, gates, w_gate, w_up, w_down):
    group_width = QUERY_HEADS // KEY_VALUE_HEADS
    query_head_rows = jnp.transpose(queries.astype(jnp.float32).reshape(SEQUENCE_LENGTH, KEY_VALUE_HEADS, group_width, HEAD_WIDTH), (1, 0, 2, 3))
    key_head_rows = jnp.transpose(keys.astype(jnp.float32).reshape(SEQUENCE_LENGTH, KEY_VALUE_HEADS, HEAD_WIDTH), (1, 0, 2))
    value_head_rows = jnp.transpose(values.astype(jnp.float32).reshape(SEQUENCE_LENGTH, KEY_VALUE_HEADS, HEAD_WIDTH), (1, 0, 2))
    heads_out = lax.map(attend_head, (query_head_rows, key_head_rows, value_head_rows))
    attn = jnp.transpose(heads_out, (2, 0, 1, 3)).reshape(SEQUENCE_LENGTH, QUERY_HEADS * HEAD_WIDTH)
    attended = (residual.astype(jnp.float32) + attn).astype(jnp.bfloat16)
    stream = attended.astype(jnp.float32)
    mean_square = lax.optimization_barrier(jnp.mean(stream * stream, axis=-1, keepdims=True))
    inverse_root = lax.rsqrt(mean_square + 1e-05)
    normed = (stream * inverse_root * norm_gain.astype(jnp.float32)).astype(jnp.bfloat16)
    blocks = N_SEQ
    assigned = TOK_DEV * TOP
    normed_blocks = normed.reshape(blocks, TOK_DEV, D)
    route_blocks = routes.reshape(blocks, assigned).astype(jnp.int32)
    one_hot = (route_blocks[:, :, None] == jnp.arange(EXPERTS, dtype=jnp.int32)[None, None, :]).astype(jnp.int32)
    before = jnp.cumsum(one_hot, axis=1) - one_hot
    slot_index = lax.optimization_barrier(jnp.sum(before * one_hot, axis=-1)).astype(jnp.int32)
    dest_slot = (route_blocks * CAP + slot_index).astype(jnp.int32)
    selected = (dest_slot[:, :, None] == jnp.arange(EXPERTS * CAP, dtype=jnp.int32)[None, None, :]).astype(jnp.int32)
    token_of = (jnp.arange(assigned, dtype=jnp.int32) // TOP)[None, :, None]
    token_index = lax.optimization_barrier(jnp.sum(selected * token_of, axis=1)).astype(jnp.int32)
    filled = lax.optimization_barrier(jnp.sum(selected, axis=1))
    slot_rows = jnp.take_along_axis(normed_blocks, token_index[:, :, None], axis=1)
    slot_rows = jnp.where(filled[:, :, None] > 0, slot_rows, jnp.zeros_like(slot_rows))
    by_expert = jnp.transpose(slot_rows.reshape(blocks, EXPERTS, CAP, D), (1, 0, 2, 3)).reshape(EXPERTS, blocks * CAP, D)
    expert_out = lax.map(expert_apply, (by_expert, w_gate, w_up, w_down))
    flat_out = expert_out.reshape(EXPERTS * blocks * CAP, D)
    block_ids = jnp.arange(blocks, dtype=jnp.int32)[:, None]
    flat_index = ((route_blocks * blocks + block_ids) * CAP + slot_index).astype(jnp.int32)
    picked = flat_out[flat_index].astype(jnp.float32).reshape(blocks, TOK_DEV, TOP, D)
    gate_blocks = gates.astype(jnp.float32).reshape(blocks, TOK_DEV, TOP)
    mixture = lax.optimization_barrier(jnp.sum(gate_blocks[..., None] * picked, axis=2)).reshape(SEQUENCE_LENGTH, D)
    layer_out = (stream + mixture).astype(jnp.bfloat16)
    return (attended, layer_out)
```

```python
import functools
import math

import jax
import jax.numpy as jnp
from jax import lax
from jax.experimental import pallas as pl
from jax.experimental.pallas import tpu as pltpu
from jax.sharding import PartitionSpec as P

D = 4096
HEAD_WIDTH = 128
GROUP = 4
TOK = 96
EXPERTS = 8
CAP = 36
PITCH = 48
PLANE = 4
ROWS = PLANE * CAP
WIDE = 512
FF_LOCAL = 448
MESH = pl.DeviceIdType.MESH
F32 = jnp.float32
BF16 = jnp.bfloat16


class Place:
    def __init__(self, depth):
        self.depth = depth
        self.half = depth // 2
        self.seq = lax.axis_index("seq")
        self.exp = lax.axis_index("exp")
        self.z = self.seq // PLANE
        self.j = lax.rem(self.seq, PLANE)
        xh, c = self.j // 2, lax.rem(self.j, 2)
        self.jp = (1 - xh) * 2 + c
        self.jc = xh * 2 + (1 - c)
        self.jcp = (1 - xh) * 2 + (1 - c)
        self.up = self.at(lax.rem(self.z + 1, depth), self.j)
        self.down = self.at(lax.rem(self.z + depth - 1, depth), self.j)
        self.partner = self.at(self.z, self.jp)
        self.sibling = self.at(self.z, self.jc)

    def at(self, z, j, e=None):
        return {"seq": z * PLANE + j, "exp": self.exp if e is None else e}


def remote(src, dst, send_sem, recv_sem, device):
    return pltpu.make_async_remote_copy(
        src_ref=src, dst_ref=dst, send_sem=send_sem, recv_sem=recv_sem,
        device_id=device, device_id_type=MESH,
    )


class Gather:
    def __init__(self, place, unit, half, sems):
        self.p, self.unit, self.cut = place, unit, half
        self.zs, self.zr, self.xs, self.xr, self.ds, self.dr = sems
        self.sent = []

    def send(self, ref, ss, rs, device):
        cp = remote(ref, ref, ss, rs, device)
        cp.start()
        self.sent.append(cp)

    def got(self, ref, rs):
        remote(ref, ref, self.zs.at[0, 0], rs, self.p.up).wait_recv()

    def ring(self, src_slot, plus, d, k, j, u):
        h = self.p.half
        sem = 2 * (d + 1) - 1 if plus else 2 * (d + 1)
        dst_slot = min(sem, 2 * h - 1)
        src, dst = self.unit(src_slot, j, u), self.unit(dst_slot, j, u)
        if d + 1 == h:
            src, dst = self.cut(src, 0 if plus else 1), self.cut(dst, 0 if plus else 1)
        cp = remote(src, dst, self.zs.at[sem, k], self.zr.at[sem, k], self.p.up if plus else self.p.down)
        cp.start()
        self.sent.append(cp)

    def across(self, slot, k, j, u):
        self.send(self.unit(slot, j, u), self.ds.at[slot, k], self.dr.at[slot, k], self.p.sibling)

    def start(self):
        p = self.p
        self.send(self.unit(0, p.j, 0), self.xs.at[8], self.xr.at[8], p.partner)
        for u in (1, 0):
            self.ring(0, True, 0, u, p.j, u)
            self.ring(0, False, 0, u, p.j, u)
        self.send(self.unit(0, p.j, 1), self.xs.at[0], self.xr.at[0], p.partner)
        self.across(0, 0, p.j, 0)
        self.across(0, 1, p.j, 1)

    def start_partner(self):
        p = self.p
        self.got(self.unit(0, p.jp, 0), self.xr.at[8])
        self.ring(0, True, 0, 2, p.jp, 0)
        self.ring(0, False, 0, 2, p.jp, 0)
        self.across(0, 2, p.jp, 0)

    def arrive(self, d):
        p, h = self.p, self.p.half
        for k, own, u in ((1, True, 1), (0, True, 0), (2, False, 0)):
            j = p.j if own else p.jp
            if d < h:
                for plus in (True, False):
                    slot = 2 * d - 1 if plus else 2 * d
                    self.got(self.unit(slot, j, u), self.zr.at[slot, k])
                    self.ring(slot, plus, d, k, j, u)
                slots = (2 * d - 1, 2 * d)
            else:
                slot = 2 * h - 1
                for part in (0, 1):
                    self.got(self.cut(self.unit(slot, j, u), part), self.zr.at[slot + part, k])
                slots = (slot,)
            for slot in slots:
                if k == 1:
                    self.send(self.unit(slot, j, 1), self.xs.at[slot], self.xr.at[slot], p.partner)
                self.across(slot, k, j, u)

    def arrive_partner(self, slots):
        for slot in slots:
            self.got(self.unit(slot, self.p.jp, 1), self.xr.at[slot])
            self.across(slot, 3, self.p.jp, 1)

    def arrive_sibling(self, slots):
        p = self.p
        for slot in slots:
            for k, (j, u) in enumerate(((p.jc, 0), (p.jc, 1), (p.jcp, 0), (p.jcp, 1))):
                self.got(self.unit(slot, j, u), self.dr.at[slot, k])

    def finish(self):
        for cp in self.sent:
            cp.wait_send()


def slots_of(d, half):
    if d == 0:
        return (0,)
    return (2 * d - 1, 2 * d) if d < half else (2 * half - 1,)


def kernel(
    depth,
    q_hbm, k_hbm, v_hbm, res_hbm, gain_hbm, routes_hbm, gates_hbm, wg_hbm, wu_hbm, wd_hbm,
    att_hbm, out_hbm,
    q_in, res_in, gain_in, routes_in, gates_in, wg, wu, wd,
    kg, vg, qs, m_s, l_s, acc_s, att, ss_buf, outgoing, rx, xg, hb, yb, dr_buf, zr_buf, xr_buf, fb, rb, ret, mixed, out_v,
    load_sem, store_sem, g_zs, g_xs, g_ds, a_zr, a_xr, a_dr, b_zr, b_xr, b_dr,
    ss_s, ss_r, x_s, x_r, c_zs, c_zr, c_xs, c_xr, c_ds, c_dr, r_s, r_r,
):
    p = Place(depth)
    half = p.half
    n_exp = EXPERTS

    def load(src, dst, i):
        cp = pltpu.make_async_copy(src, dst, load_sem.at[i])
        cp.start()
        return cp

    loads = [
        load(k_hbm, kg.at[0, p.j], 0), load(v_hbm, vg.at[0, p.j], 1), load(q_hbm, q_in, 2),
        load(res_hbm, res_in, 3), load(gain_hbm, gain_in, 4), load(routes_hbm, routes_in, 5),
        load(gates_hbm, gates_in, 6),
    ]

    barrier = pltpu.get_barrier_semaphore()

    def greet(device):
        pl.semaphore_signal(barrier, inc=1, device_id=device, device_id_type=MESH)

    for device in (p.up, p.down, p.partner, p.sibling):
        greet(device)
    for i in range(1, n_exp):
        greet(p.at(p.z, p.j, lax.rem(p.exp + i, n_exp)))
    home = p.exp // 2
    mine = home == p.j
    for i in range(n_exp):
        f = lax.rem(p.exp + i, n_exp)
        if i == 0:
            @pl.when(jnp.logical_not(mine))
            def _():
                greet(p.at(p.z, home, f))
        else:
            greet(p.at(p.z, home, f))
    for u in range(2):
        for jj in range(PLANE):
            src_e = 2 * p.j + u

            @pl.when(jnp.logical_not(jnp.logical_and(jj == p.j, src_e == p.exp)))
            def _():
                greet(p.at(p.z, jj, src_e))
    pl.semaphore_wait(barrier, 4 + (n_exp - 1) + 16 - 2 * mine.astype(jnp.int32))

    loads[0].wait()
    loads[1].wait()

    def kv_unit(slot, j, u):
        return (vg if u else kg).at[slot, j]

    kv = Gather(p, kv_unit, lambda r, part: r.at[pl.ds(part * (TOK // 2), TOK // 2)], (g_zs, a_zr, g_xs, a_xr, g_ds, a_dr))
    kv.start()

    weight_loads = [load(wg_hbm, wg, 7), load(wu_hbm, wu, 8), load(wd_hbm, wd, 9)]
    for cp in loads[2:]:
        cp.wait()

    for h in range(GROUP):
        qs[pl.ds(h * TOK, TOK), :] = q_in[:, h * HEAD_WIDTH:(h + 1) * HEAD_WIDTH]

    kv.start_partner()

    r_row = [routes_in[k:k + 1, :] for k in range(2)]
    expert_ids = lax.broadcasted_iota(jnp.int32, (EXPERTS, TOK), 0)
    one_hot = [(expert_ids == r_row[k]).astype(F32) for k in range(2)]
    earlier = (
        lax.broadcasted_iota(jnp.int32, (TOK, TOK), 0) < lax.broadcasted_iota(jnp.int32, (TOK, TOK), 1)
    ).astype(BF16)
    before = jnp.dot((one_hot[0] + one_hot[1]).astype(BF16), earlier, preferred_element_type=F32)
    slot_row = [jnp.sum(one_hot[k] * before, axis=0, keepdims=True) for k in range(2)]
    dest = [r_row[k] * PITCH + slot_row[k].astype(jnp.int32) for k in range(2)]
    slot_ids = lax.broadcasted_iota(jnp.int32, (EXPERTS * PITCH, TOK), 0)
    match = [slot_ids == dest[k] for k in range(2)]
    dispatch = jnp.where(jnp.logical_or(match[0], match[1]), 1.0, 0.0).astype(F32)
    mixed[...] = jnp.where(match[0], gates_in[0:1, :], 0.0) + jnp.where(match[1], gates_in[1:2, :], 0.0)

    scale = 1.0 / math.sqrt(HEAD_WIDTH)
    kv_rows = PLANE * TOK

    def attend(slot, first):
        keys = kg[slot].reshape(kv_rows, HEAD_WIDTH)
        vals = vg[slot].reshape(kv_rows, HEAD_WIDTH)
        scores = lax.dot_general(qs[...], keys, (((1,), (1,)), ((), ())), preferred_element_type=F32) * scale
        if first:
            at = lax.broadcasted_iota(jnp.int32, scores.shape, 0)
            for h in range(1, GROUP):
                at = at - jnp.where(lax.broadcasted_iota(jnp.int32, scores.shape, 0) >= h * TOK, TOK, 0)
            seen = lax.broadcasted_iota(jnp.int32, scores.shape, 1) <= at + p.j * TOK
            scores = jnp.where(seen, scores, -1e30)
            top = jnp.max(scores, axis=1, keepdims=True)
            terms = jnp.where(seen, jnp.exp(scores - top), 0.0)
            m_s[...] = top
            l_s[...] = jnp.sum(terms, axis=1, keepdims=True)
            acc_s[...] = jnp.dot(terms.astype(BF16), vals, preferred_element_type=F32)
        else:
            old = m_s[...]
            top = jnp.maximum(old, jnp.max(scores, axis=1, keepdims=True))
            fade = jnp.exp(old - top)
            terms = jnp.exp(scores - top)
            m_s[...] = top
            l_s[...] = l_s[...] * fade + jnp.sum(terms, axis=1, keepdims=True)
            acc_s[...] = acc_s[...] * fade + jnp.dot(terms.astype(BF16), vals, preferred_element_type=F32)

    def attend_all(d):
        for slot in slots_of(d, half):
            if slot == 0:
                attend(0, True)
            else:
                if d == half:
                    seen = p.z >= half
                elif slot % 2 == 1:
                    seen = p.z >= d
                else:
                    seen = p.z + d >= depth

                @pl.when(seen)
                def _(slot=slot):
                    attend(slot, False)

    for d in range(1, half + 1):
        kv.arrive(d)
        kv.arrive_partner(slots_of(d - 1, half))
        kv.arrive_sibling(slots_of(d - 1, half))
        attend_all(d - 1)
    kv.arrive_partner(slots_of(half, half))
    kv.arrive_sibling(slots_of(half, half))
    attend_all(half)

    for h in range(GROUP):
        rows, cols = slice(h * TOK, (h + 1) * TOK), slice(h * HEAD_WIDTH, (h + 1) * HEAD_WIDTH)
        att[:, cols] = (res_in[:, cols].astype(F32) + acc_s[rows, :] / l_s[rows, :]).astype(BF16)
    att_store = pltpu.make_async_copy(att, att_hbm, store_sem.at[0])
    att_store.start()

    stream = att[...].astype(F32)
    squares = lax.dot_general(
        jnp.ones((8, WIDE), F32), stream * stream, (((1,), (1,)), ((), ())),
        precision=lax.Precision.HIGHEST, preferred_element_type=F32,
    )
    ss_buf[p.exp, :, pl.ds(0, TOK)] = squares
    ss_sends = []
    for i in range(1, n_exp):
        other = lax.rem(p.exp + i, n_exp)
        cp = remote(ss_buf.at[p.exp], ss_buf.at[p.exp], ss_s.at[i], ss_r.at[i], p.at(p.z, p.j, other))
        cp.start()
        ss_sends.append(cp)
    rows_out = jnp.dot(dispatch.astype(BF16), att[...], preferred_element_type=F32)
    for i in range(1, n_exp):
        other = lax.rem(p.exp + n_exp - i, n_exp)
        remote(ss_buf.at[other], ss_buf.at[other], ss_s.at[i], ss_r.at[i], p.up).wait_recv()
    total = ss_buf[0, :, pl.ds(0, TOK)]
    for i in range(1, n_exp):
        total = total + ss_buf[i, :, pl.ds(0, TOK)]
    inverse = lax.rsqrt(total / D + 1e-05)
    columns = lax.dot_general(
        dispatch, inverse, (((1,), (1,)), ((), ())), precision=lax.Precision.HIGHEST, preferred_element_type=F32
    )
    normed = (rows_out * columns[:, 0:1] * gain_in[...]).astype(BF16)
    outgoing[...] = normed.reshape(EXPERTS, PITCH, WIDE)

    u_me = lax.rem(p.exp, 2)
    x_sends = []
    for i in range(n_exp):
        f = lax.rem(p.exp + i, n_exp)
        cp = remote(outgoing.at[f], rx.at[u_me, p.j], x_s.at[i], x_r.at[u_me, p.j], p.at(p.z, home, f))
        x_sends.append(cp)
        if i == 0:
            pl.when(jnp.logical_not(mine))(cp.start)

            @pl.when(mine)
            def _():
                rx[u_me, p.j] = outgoing[p.exp]
        else:
            cp.start()

    kv.finish()

    row_ids = lax.broadcasted_iota(jnp.int32, (ROWS, PLANE * PITCH), 0)
    for i in range(1, PLANE):
        row_ids = row_ids + jnp.where(
            lax.broadcasted_iota(jnp.int32, (ROWS, PLANE * PITCH), 0) >= i * CAP, PITCH - CAP, 0
        )
    pack = (row_ids == lax.broadcasted_iota(jnp.int32, (ROWS, PLANE * PITCH), 1)).astype(BF16)

    def columns_of(j, u):
        return pl.ds(pl.multiple_of(j * (2 * WIDE) + u * WIDE, WIDE), WIDE)

    for u in range(2):
        for jj in range(PLANE):
            here = jnp.logical_and(jj == p.j, 2 * p.j + u == p.exp)

            @pl.when(jnp.logical_not(here))
            def _(u=u, jj=jj):
                remote(rx.at[u, jj], rx.at[u, jj], x_s.at[0], x_r.at[u, jj], p.up).wait_recv()

        packed = jnp.dot(pack, rx[u].reshape(PLANE * PITCH, WIDE), preferred_element_type=F32)
        xg[0, :, columns_of(p.j, u)] = packed.astype(BF16)

    def row_unit(slot, j, u):
        return xg.at[slot, :, columns_of(j, u)]

    def row_half(ref, part):
        return ref.at[pl.ds(part * 80, 80 if part == 0 else ROWS - 80)]

    ag = Gather(p, row_unit, row_half, (g_zs, b_zr, g_xs, b_xr, g_ds, b_dr))
    ag.start()
    for cp in weight_loads:
        cp.wait()
    ag.start_partner()

    def hidden(lo, hi):
        count = hi - lo
        rows = xg[lo:hi].reshape(count * ROWS, D)
        gate = jnp.dot(rows, wg[...], preferred_element_type=F32)
        up = jnp.dot(rows, wu[...], preferred_element_type=F32)
        act = gate / (1.0 + jnp.exp(-gate)) * up
        hb[lo:hi] = act.astype(BF16).reshape(count, ROWS, FF_LOCAL)

    def hidden_all(d):
        slots = slots_of(d, half)
        hidden(slots[0], slots[-1] + 1)

    for d in range(1, half + 1):
        ag.arrive(d)
        ag.arrive_partner(slots_of(d - 1, half))
        ag.arrive_sibling(slots_of(d - 1, half))
        hidden_all(d - 1)
    ag.arrive_partner(slots_of(half, half))
    ag.arrive_sibling(slots_of(half, half))
    hidden_all(half)

    sent = []

    def send(src, dst, ss, rs, device):
        cp = remote(src, dst, ss, rs, device)
        cp.start()
        sent.append(cp)

    def wait_for(ref, rs):
        remote(ref, ref, c_zs.at[0, 0], rs, p.up).wait_recv()

    def wide_columns(j):
        return pl.ds(pl.multiple_of(j * (2 * WIDE), 2 * WIDE), 2 * WIDE)

    def produce(slot):
        def part(n, _):
            cols = pl.ds(pl.multiple_of(n * WIDE, WIDE), WIDE)
            yb[slot, :, cols] = jnp.dot(hb[slot], wd[:, cols], preferred_element_type=F32).astype(BF16)
            return 0

        lax.fori_loop(0, D // WIDE, part, 0)
        for k, j in enumerate((p.jc, p.jcp)):
            send(yb.at[slot, :, wide_columns(j)], dr_buf.at[slot, k], c_ds.at[slot, k], c_dr.at[slot, k], p.sibling)

    def for_partner(slot):
        for k in range(2):
            wait_for(dr_buf.at[slot, k], c_dr.at[slot, k])
        cols = columns_of(p.jp, 1)
        yb[slot, :, cols] = (yb[slot, :, cols].astype(F32) + dr_buf[slot, 1, :, WIDE:].astype(F32)).astype(BF16)
        send(yb.at[slot, :, cols], xr_buf.at[slot], c_xs.at[slot], c_xr.at[slot], p.partner)

    def halves(ref, part):
        return ref.at[:, pl.ds(part * (WIDE // 2), WIDE // 2)]

    def reduce_slot(slot, d):
        for k, j, u in ((0, p.j, 0), (2, p.jp, 0), (1, p.j, 1)):
            cols = columns_of(j, u)
            own = k != 2
            total = yb[slot, :, cols].astype(F32)
            total = total + dr_buf[slot, 0 if own else 1, :, pl.ds(u * WIDE, WIDE)].astype(F32)
            if k == 1:
                wait_for(xr_buf.at[slot], c_xr.at[slot])
                total = total + xr_buf[slot].astype(F32)
            if d == half:
                yb[slot, :, cols] = total.astype(BF16)
            elif d == half - 1:
                part = 0 if slot % 2 == 1 else 1
                wait_for(halves(zr_buf.at[slot, k], part), c_zr.at[slot, k])
                cut = slice(part * (WIDE // 2), (part + 1) * (WIDE // 2))
                keep = slice((1 - part) * (WIDE // 2), (2 - part) * (WIDE // 2))
                zr = zr_buf[slot, k, :, cut].astype(F32)
                base = j * (2 * WIDE) + u * WIDE
                for piece, value in ((cut, total[:, cut] + zr), (keep, total[:, keep])):
                    at = pl.ds(pl.multiple_of(base + piece.start, WIDE // 2), WIDE // 2)
                    yb[slot, :, at] = value.astype(BF16)
            else:
                sources = (0, 2 * half - 1) if slot == 0 else (slot,)
                for i in sources:
                    wait_for(zr_buf.at[i, k], c_zr.at[i, k])
                    total = total + zr_buf[i, k].astype(F32)
                yb[slot, :, cols] = total.astype(BF16)
            if d == 0:
                if k == 2:
                    send(yb.at[slot, :, cols], xr_buf.at[8], c_xs.at[8], c_xr.at[8], p.partner)
            elif d == half:
                for part in (0, 1):
                    to = 2 * (d - 1) - 1 + part
                    base = j * (2 * WIDE) + u * WIDE + part * (WIDE // 2)
                    send(
                        yb.at[slot, :, pl.ds(pl.multiple_of(base, WIDE // 2), WIDE // 2)],
                        halves(zr_buf.at[to, k], part),
                        c_zs.at[slot + part, k], c_zr.at[to, k], p.down if part == 0 else p.up,
                    )
            else:
                plus = slot % 2 == 1
                if d == 1:
                    to = 0 if plus else 2 * half - 1
                else:
                    to = slot - 2
                send(
                    yb.at[slot, :, cols], zr_buf.at[to, k], c_zs.at[slot, k], c_zr.at[to, k],
                    p.down if plus else p.up,
                )

    order = [(d, s) for d in range(half, -1, -1) for s in slots_of(d, half)]
    produce(order[0][1])
    for d in range(half, -1, -1):
        ahead = slots_of(d - 1, half) if d > 0 else ()
        for s in slots_of(d, half):
            for_partner(s)
        for s in ahead:
            produce(s)
        for s in slots_of(d, half):
            reduce_slot(s, d)

    wait_for(xr_buf.at[8], c_xr.at[8])
    first = columns_of(p.j, 0)
    fb[0] = (yb[0, :, first].astype(F32) + xr_buf[8].astype(F32)).astype(BF16)
    fb[1] = yb[0, :, columns_of(p.j, 1)]

    for u in range(2):
        spread = lax.dot_general(pack, fb[u], (((0,), (0,)), ((), ())), preferred_element_type=F32)
        rb[u] = spread.astype(BF16).reshape(PLANE, PITCH, WIDE)
    r_sends = []
    for u in range(2):
        for jj in range(PLANE):
            here = jnp.logical_and(jj == p.j, 2 * p.j + u == p.exp)
            cp = remote(rb.at[u, jj], ret.at[p.exp], r_s.at[u * PLANE + jj], r_r.at[p.exp], p.at(p.z, jj, 2 * p.j + u))
            r_sends.append((here, cp))
            pl.when(jnp.logical_not(here))(cp.start)

            @pl.when(here)
            def _(u=u, jj=jj):
                ret[p.exp] = rb[u, jj]

    ag.finish()
    for cp in sent:
        cp.wait_send()
    for cp in ss_sends:
        cp.wait_send()
    for i, cp in enumerate(x_sends):
        if i == 0:
            pl.when(jnp.logical_not(mine))(cp.wait_send)
        else:
            cp.wait_send()

    for i in range(n_exp):
        f = lax.rem(p.exp + i, n_exp)
        cp = remote(ret.at[f], ret.at[f], r_s.at[0], r_r.at[f], p.up)
        if i == 0:
            pl.when(jnp.logical_not(mine))(cp.wait_recv)
        else:
            cp.wait_recv()
    returned = ret[...].reshape(EXPERTS * PITCH, WIDE).astype(F32)
    mix = lax.dot_general(
        mixed[...], returned, (((0,), (0,)), ((), ())), precision=lax.Precision.HIGHEST, preferred_element_type=F32
    )
    out_v[...] = (att[...].astype(F32) + mix).astype(BF16)
    out_store = pltpu.make_async_copy(out_v, out_hbm, store_sem.at[1])
    out_store.start()
    for here, cp in r_sends:
        pl.when(jnp.logical_not(here))(cp.wait_send)
    att_store.wait()
    out_store.wait()


def shards(depth, queries, keys, values, residual, norm_gain, routes, gates, w_gate, w_up, w_down):
    any_spec = pl.BlockSpec(memory_space=pl.ANY)
    slots = depth
    vmem, dma = pltpu.VMEM, pltpu.SemaphoreType.DMA
    tok_block = jax.ShapeDtypeStruct((TOK, WIDE), BF16)
    scratch = [
        vmem((TOK, WIDE), BF16), vmem((TOK, WIDE), BF16), vmem((1, WIDE), F32), vmem((2, TOK), jnp.int32),
        vmem((2, TOK), F32), vmem((D, FF_LOCAL), BF16), vmem((D, FF_LOCAL), BF16), vmem((FF_LOCAL, D), BF16),
        vmem((slots, PLANE, TOK, HEAD_WIDTH), BF16), vmem((slots, PLANE, TOK, HEAD_WIDTH), BF16),
        vmem((GROUP * TOK, HEAD_WIDTH), BF16), vmem((GROUP * TOK, 1), F32), vmem((GROUP * TOK, 1), F32),
        vmem((GROUP * TOK, HEAD_WIDTH), F32), vmem((TOK, WIDE), BF16), vmem((EXPERTS, 8, 128), F32),
        vmem((EXPERTS, PITCH, WIDE), BF16), vmem((2, PLANE, PITCH, WIDE), BF16),
        vmem((slots, ROWS, D), BF16), vmem((slots, ROWS, FF_LOCAL), BF16), vmem((slots, ROWS, D), BF16),
        vmem((slots, 2, ROWS, 2 * WIDE), BF16), vmem((slots, 3, ROWS, WIDE), BF16), vmem((9, ROWS, WIDE), BF16),
        vmem((2, ROWS, WIDE), BF16), vmem((2, PLANE, PITCH, WIDE), BF16), vmem((EXPERTS, PITCH, WIDE), BF16),
        vmem((EXPERTS * PITCH, TOK), F32), vmem((TOK, WIDE), BF16),
        dma((10,)), dma((2,)),
        dma((9, 3)), dma((9,)), dma((8, 4)),
        dma((9, 3)), dma((9,)), dma((8, 4)),
        dma((9, 3)), dma((9,)), dma((8, 4)),
        dma((8,)), dma((8,)), dma((8,)), dma((2, PLANE)),
        dma((9, 3)), dma((9, 3)), dma((9,)), dma((9,)), dma((8, 2)), dma((8, 2)),
        dma((8,)), dma((8,)),
    ]
    return pl.pallas_call(
        functools.partial(kernel, depth),
        out_shape=(tok_block, tok_block),
        in_specs=[any_spec] * 10,
        out_specs=(any_spec, any_spec),
        scratch_shapes=scratch,
        compiler_params=pltpu.CompilerParams(
            collective_id=0, has_side_effects=True, vmem_limit_bytes=64 * 1024 * 1024 - 65536
        ),
    )(
        queries, keys, values, residual, norm_gain.reshape(1, WIDE), routes.T, gates.T,
        w_gate[0], w_up[0], w_down[0],
    )


def solution(mesh):
    in_specs = (
        P("seq", "exp"), P("seq", "exp"), P("seq", "exp"), P("seq", "exp"), P("exp"), P("seq", None), P("seq", None),
        P("exp", None, "seq"), P("exp", None, "seq"), P("exp", "seq", None),
    )
    body = functools.partial(shards, mesh.shape["seq"] // PLANE)
    return jax.shard_map(body, mesh=mesh, in_specs=in_specs, out_specs=(P("seq", "exp"), P("seq", "exp")), check_vma=False)
```

```python
import functools
import math

import jax
import jax.numpy as jnp
from jax import lax
from jax.experimental import pallas as pl
from jax.experimental.pallas import tpu as pltpu
from jax.sharding import PartitionSpec as P

D = 4096
HEAD_WIDTH = 128
GROUP = 4
TOK = 96
EXPERTS = 8
CAP = 36
PITCH = 48
PLANE = 4
ROWS = PLANE * CAP
WIDE = 512
FF_LOCAL = 448
MESH = pl.DeviceIdType.MESH
VMEM_BYTES = 63 * 1024 * 1024
F32 = jnp.float32
BF16 = jnp.bfloat16


class Place:
    def __init__(self, depth):
        self.depth = depth
        self.half = depth // 2
        self.seq = lax.axis_index("seq")
        self.exp = lax.axis_index("exp")
        self.z = self.seq // PLANE
        self.j = lax.rem(self.seq, PLANE)
        xh, c = self.j // 2, lax.rem(self.j, 2)
        self.jp = (1 - xh) * 2 + c
        self.jc = xh * 2 + (1 - c)
        self.jcp = (1 - xh) * 2 + (1 - c)
        self.up = self.at(lax.rem(self.z + 1, depth), self.j)
        self.down = self.at(lax.rem(self.z + depth - 1, depth), self.j)
        self.up_other = self.at(lax.rem(self.z + 1, depth), self.jp)
        self.down_other = self.at(lax.rem(self.z + depth - 1, depth), self.jp)
        self.partner = self.at(self.z, self.jp)
        self.sibling = self.at(self.z, self.jc)

    def at(self, z, j, e=None):
        return {"seq": z * PLANE + j, "exp": self.exp if e is None else e}


def remote(src, dst, send_sem, recv_sem, device):
    return pltpu.make_async_remote_copy(
        src_ref=src, dst_ref=dst, send_sem=send_sem, recv_sem=recv_sem,
        device_id=device, device_id_type=MESH,
    )


class Gather:
    def __init__(self, place, unit, half, sems):
        self.p, self.unit, self.cut = place, unit, half
        self.zs, self.zr, self.xs, self.xr, self.ds, self.dr = sems
        self.sent = []

    def send(self, ref, ss, rs, device):
        cp = remote(ref, ref, ss, rs, device)
        cp.start()
        self.sent.append(cp)

    def got(self, ref, rs):
        remote(ref, ref, self.zs.at[0, 0], rs, self.p.up).wait_recv()

    def ring(self, src_slot, plus, d, k, j, u):
        h = self.p.half
        sem = 2 * (d + 1) - 1 if plus else 2 * (d + 1)
        dst_slot = min(sem, 2 * h - 1)
        src, dst = self.unit(src_slot, j, u), self.unit(dst_slot, j, u)
        if d + 1 == h:
            src, dst = self.cut(src, 0 if plus else 1), self.cut(dst, 0 if plus else 1)
        cp = remote(src, dst, self.zs.at[sem, k], self.zr.at[sem, k], self.p.up if plus else self.p.down)
        cp.start()
        self.sent.append(cp)

    def across(self, slot, k, j, u):
        self.send(self.unit(slot, j, u), self.ds.at[slot, k], self.dr.at[slot, k], self.p.sibling)

    def start(self, u):
        p = self.p
        if u == 0:
            self.send(self.unit(0, p.j, 0), self.xs.at[8], self.xr.at[8], p.partner)
        self.ring(0, True, 0, u, p.j, u)
        self.ring(0, False, 0, u, p.j, u)
        self.across(0, u, p.j, u)
        if u == 0:
            self.send(self.unit(0, p.j, 1), self.xs.at[0], self.xr.at[0], p.partner)

    def start_partner(self):
        p = self.p
        self.got(self.unit(0, p.jp, 0), self.xr.at[8])
        self.ring(0, True, 0, 2, p.jp, 0)
        self.ring(0, False, 0, 2, p.jp, 0)
        self.across(0, 2, p.jp, 0)

    def arrive(self, d, after):
        p, h = self.p, self.p.half
        for k, own, u in ((1, True, 1), (0, True, 0), (2, False, 0)):
            j = p.j if own else p.jp
            if d < h:
                for plus in (True, False):
                    slot = 2 * d - 1 if plus else 2 * d
                    self.got(self.unit(slot, j, u), self.zr.at[slot, k])
                    self.ring(slot, plus, d, k, j, u)
                slots = (2 * d - 1, 2 * d)
            else:
                slot = 2 * h - 1
                for part in (0, 1):
                    self.got(self.cut(self.unit(slot, j, u), part), self.zr.at[slot + part, k])
                slots = (slot,)
            for slot in slots:
                if k == 1:
                    self.send(self.unit(slot, j, 1), self.xs.at[slot], self.xr.at[slot], p.partner)
                self.across(slot, k, j, u)
            after(k)

    def arrive_partner(self, slots):
        for slot in slots:
            self.got(self.unit(slot, self.p.jp, 1), self.xr.at[slot])
            self.across(slot, 3, self.p.jp, 1)

    def arrive_sibling(self, slots):
        p = self.p
        for slot in slots:
            for k, (j, u) in enumerate(((p.jc, 0), (p.jc, 1), (p.jcp, 0), (p.jcp, 1))):
                self.got(self.unit(slot, j, u), self.dr.at[slot, k])

    def finish(self):
        for cp in self.sent:
            cp.wait_send()


class KvGather:
    def __init__(self, place, kv, sems):
        self.p, self.kv = place, kv
        self.zs, self.zr, self.xs, self.xr, self.ds, self.dr = sems
        self.sent = []

    def send(self, ref, ss, rs, device):
        cp = remote(ref, ref, ss, rs, device)
        cp.start()
        self.sent.append(cp)

    def got(self, ref, rs):
        remote(ref, ref, self.zs.at[0, 0], rs, self.p.up).wait_recv()

    def ring(self, src_slot, plus, d, k):
        p, h = self.p, self.p.half
        sem = 2 * (d + 1) - 1 if plus else 2 * (d + 1)
        src, dst = self.kv.at[src_slot, p.j], self.kv.at[min(sem, 2 * h - 1), p.j]
        if d + 1 == h:
            part = 0 if plus else 1
            src, dst = src.at[part], dst.at[part]
        device = ((p.up, p.up_other) if plus else (p.down, p.down_other))[k]
        cp = remote(src, dst, self.zs.at[sem, k], self.zr.at[sem, k], device)
        cp.start()
        self.sent.append(cp)

    def across(self, slot, k, j):
        self.send(self.kv.at[slot, j], self.ds.at[slot, k], self.dr.at[slot, k], self.p.sibling)

    def start(self):
        p = self.p
        for k in (0, 1):
            self.ring(0, True, 0, k)
            self.ring(0, False, 0, k)
        self.send(self.kv.at[0, p.j], self.xs.at[0], self.xr.at[0], p.partner)
        self.across(0, 0, p.j)

    def arrive(self, d):
        p, h = self.p, self.p.half
        for slot in slots_of(d, h):
            if d < h:
                self.got(self.kv.at[slot, p.j], self.zr.at[slot, 0])
                for k in (0, 1):
                    self.ring(slot, slot % 2 == 1, d, k)
            else:
                for part in (0, 1):
                    self.got(self.kv.at[slot, p.j, part], self.zr.at[slot + part, 0])
            self.across(slot, 0, p.j)

    def arrive_other(self, d):
        p, h = self.p, self.p.half
        for slot in slots_of(d, h):
            if d == 0:
                self.got(self.kv.at[slot, p.jp], self.xr.at[0])
            elif d < h:
                self.got(self.kv.at[slot, p.jp], self.zr.at[slot, 1])
            else:
                for part in (0, 1):
                    self.got(self.kv.at[slot, p.jp, part], self.zr.at[slot + part, 1])
            self.across(slot, 1, p.jp)

    def arrive_sibling(self, slots):
        p = self.p
        for slot in slots:
            for k, j in enumerate((p.jc, p.jcp)):
                self.got(self.kv.at[slot, j], self.dr.at[slot, k])

    def finish(self):
        for cp in self.sent:
            cp.wait_send()


def slots_of(d, half):
    if d == 0:
        return (0,)
    return (2 * d - 1, 2 * d) if d < half else (2 * half - 1,)


def kernel(
    depth,
    q_hbm, k_hbm, v_hbm, res_hbm, gain_hbm, routes_hbm, gates_hbm, wg_hbm, wu_hbm, wd_hbm,
    attn_out, mix_out,
    q_in, res_in, gain_in, routes_in, gates_in, wg, wu, wd,
    kvg, qs, m_s, l_s, acc_s, att, ss_buf, outgoing, rx, xg, hb, yb, dr_buf, zr_buf, xr_buf, fb, rb, ret, mixed,
    load_sem, g_zs, g_xs, g_ds, a_zr, a_xr, a_dr, b_zr, b_xr, b_dr,
    ss_s, ss_r, x_s, x_r, c_zs, c_zr, c_xs, c_xr, c_ds, c_dr, r_s, r_r,
):
    p = Place(depth)
    half = p.half
    n_exp = EXPERTS

    def load(src, dst, i):
        cp = pltpu.make_async_copy(src, dst, load_sem.at[i])
        cp.start()
        return cp

    loads = [
        load(k_hbm, kvg.at[0, p.j, 0], 0), load(v_hbm, kvg.at[0, p.j, 1], 1), load(q_hbm, q_in, 2),
        load(res_hbm, res_in, 3), load(gain_hbm, gain_in, 4), load(routes_hbm, routes_in, 5),
        load(gates_hbm, gates_in, 6),
    ]

    barrier = pltpu.get_barrier_semaphore()

    def greet(device):
        pl.semaphore_signal(barrier, inc=1, device_id=device, device_id_type=MESH)

    for device in (p.up, p.down, p.up_other, p.down_other, p.partner, p.sibling):
        greet(device)
    for i in range(1, n_exp):
        greet(p.at(p.z, p.j, lax.rem(p.exp + i, n_exp)))
    home = p.exp // 2
    mine = home == p.j
    for i in range(n_exp):
        f = lax.rem(p.exp + i, n_exp)
        if i == 0:
            @pl.when(jnp.logical_not(mine))
            def _():
                greet(p.at(p.z, home, f))
        else:
            greet(p.at(p.z, home, f))
    for u in range(2):
        for jj in range(PLANE):
            src_e = 2 * p.j + u

            @pl.when(jnp.logical_not(jnp.logical_and(jj == p.j, src_e == p.exp)))
            def _():
                greet(p.at(p.z, jj, src_e))
    pl.semaphore_wait(barrier, 6 + (n_exp - 1) + 16 - 2 * mine.astype(jnp.int32))

    loads[0].wait()
    loads[1].wait()

    kv = KvGather(p, kvg, (g_zs, a_zr, g_xs, a_xr, g_ds, a_dr))
    kv.start()

    weight_loads = [load(wg_hbm, wg, 7), load(wu_hbm, wu, 8), load(wd_hbm, wd, 9)]
    for cp in loads[2:]:
        cp.wait()

    for h in range(GROUP):
        qs[pl.ds(h * TOK, TOK), :] = q_in[:, h * HEAD_WIDTH:(h + 1) * HEAD_WIDTH]

    r_row = [routes_in[k:k + 1, :] for k in range(2)]
    expert_ids = lax.broadcasted_iota(jnp.int32, (EXPERTS, TOK), 0)
    one_hot = [(expert_ids == r_row[k]).astype(F32) for k in range(2)]
    earlier = (
        lax.broadcasted_iota(jnp.int32, (TOK, TOK), 0) < lax.broadcasted_iota(jnp.int32, (TOK, TOK), 1)
    ).astype(BF16)
    before = jnp.dot((one_hot[0] + one_hot[1]).astype(BF16), earlier, preferred_element_type=F32)
    slot_row = [jnp.sum(one_hot[k] * before, axis=0, keepdims=True) for k in range(2)]
    dest = [r_row[k] * PITCH + slot_row[k].astype(jnp.int32) for k in range(2)]
    slot_ids = lax.broadcasted_iota(jnp.int32, (EXPERTS * PITCH, TOK), 0)
    match = [slot_ids == dest[k] for k in range(2)]
    dispatch = jnp.where(jnp.logical_or(match[0], match[1]), 1.0, 0.0).astype(F32)
    mixed[...] = jnp.where(match[0], gates_in[0:1, :], 0.0) + jnp.where(match[1], gates_in[1:2, :], 0.0)

    scale = 1.0 / math.sqrt(HEAD_WIDTH)
    kv_rows = PLANE * TOK

    def attend(slot, first):
        keys = kvg[slot, :, 0].reshape(kv_rows, HEAD_WIDTH)
        vals = kvg[slot, :, 1].reshape(kv_rows, HEAD_WIDTH)
        scores = lax.dot_general(qs[...], keys, (((1,), (1,)), ((), ())), preferred_element_type=F32) * scale
        if first:
            at = lax.broadcasted_iota(jnp.int32, scores.shape, 0)
            for h in range(1, GROUP):
                at = at - jnp.where(lax.broadcasted_iota(jnp.int32, scores.shape, 0) >= h * TOK, TOK, 0)
            seen = lax.broadcasted_iota(jnp.int32, scores.shape, 1) <= at + p.j * TOK
            scores = jnp.where(seen, scores, -1e30)
            top = jnp.max(scores, axis=1, keepdims=True)
            terms = jnp.where(seen, jnp.exp(scores - top), 0.0)
            m_s[...] = top
            l_s[...] = jnp.sum(terms, axis=1, keepdims=True)
            acc_s[...] = jnp.dot(terms.astype(BF16), vals, preferred_element_type=F32)
        else:
            old = m_s[...]
            top = jnp.maximum(old, jnp.max(scores, axis=1, keepdims=True))
            fade = jnp.exp(old - top)
            terms = jnp.exp(scores - top)
            m_s[...] = top
            l_s[...] = l_s[...] * fade + jnp.sum(terms, axis=1, keepdims=True)
            acc_s[...] = acc_s[...] * fade + jnp.dot(terms.astype(BF16), vals, preferred_element_type=F32)

    def attend_all(d):
        for slot in slots_of(d, half):
            if slot == 0:
                attend(0, True)
            else:
                if d == half:
                    seen = p.z >= half
                elif slot % 2 == 1:
                    seen = p.z >= d
                else:
                    seen = p.z + d >= depth

                @pl.when(seen)
                def _(slot=slot):
                    attend(slot, False)

    for d in range(1, half + 1):
        kv.arrive(d)
        kv.arrive_other(d - 1)
        kv.arrive_sibling(slots_of(d - 1, half))
        attend_all(d - 1)
    kv.arrive_other(half)
    kv.arrive_sibling(slots_of(half, half))
    attend_all(half)

    for h in range(GROUP):
        rows, cols = slice(h * TOK, (h + 1) * TOK), slice(h * HEAD_WIDTH, (h + 1) * HEAD_WIDTH)
        attn = acc_s[rows, :] / l_s[rows, :]
        attn_out[:, cols] = attn
        att[:, cols] = (res_in[:, cols].astype(F32) + attn).astype(BF16)

    stream = att[...].astype(F32)
    squares = lax.dot_general(
        jnp.ones((8, WIDE), F32), stream * stream, (((1,), (1,)), ((), ())),
        precision=lax.Precision.HIGHEST, preferred_element_type=F32,
    )
    ss_buf[p.exp, :, pl.ds(0, TOK)] = squares
    ss_sends = []
    for i in range(1, n_exp):
        other = lax.rem(p.exp + i, n_exp)
        cp = remote(ss_buf.at[p.exp], ss_buf.at[p.exp], ss_s.at[i], ss_r.at[i], p.at(p.z, p.j, other))
        cp.start()
        ss_sends.append(cp)
    rows_out = jnp.dot(dispatch.astype(BF16), att[...], preferred_element_type=F32)
    for i in range(1, n_exp):
        other = lax.rem(p.exp + n_exp - i, n_exp)
        remote(ss_buf.at[other], ss_buf.at[other], ss_s.at[i], ss_r.at[i], p.up).wait_recv()
    total = ss_buf[0, :, pl.ds(0, TOK)]
    for i in range(1, n_exp):
        total = total + ss_buf[i, :, pl.ds(0, TOK)]
    inverse = lax.rsqrt(total / D + 1e-05)
    columns = lax.dot_general(
        dispatch, inverse, (((1,), (1,)), ((), ())), precision=lax.Precision.HIGHEST, preferred_element_type=F32
    )
    normed = (rows_out * columns[:, 0:1] * gain_in[...]).astype(BF16)
    outgoing[...] = normed.reshape(EXPERTS, PITCH, WIDE)

    u_me = lax.rem(p.exp, 2)
    x_sends = []
    for i in range(n_exp):
        f = lax.rem(p.exp + i, n_exp)
        cp = remote(outgoing.at[f], rx.at[u_me, p.j], x_s.at[i], x_r.at[u_me, p.j], p.at(p.z, home, f))
        x_sends.append(cp)
        if i == 0:
            pl.when(jnp.logical_not(mine))(cp.start)

            @pl.when(mine)
            def _():
                rx[u_me, p.j] = outgoing[p.exp]
        else:
            cp.start()

    kv.finish()

    row_ids = lax.broadcasted_iota(jnp.int32, (ROWS, PLANE * PITCH), 0)
    for i in range(1, PLANE):
        row_ids = row_ids + jnp.where(
            lax.broadcasted_iota(jnp.int32, (ROWS, PLANE * PITCH), 0) >= i * CAP, PITCH - CAP, 0
        )
    pack = (row_ids == lax.broadcasted_iota(jnp.int32, (ROWS, PLANE * PITCH), 1)).astype(BF16)

    def columns_of(j, u):
        return pl.ds(pl.multiple_of(j * (2 * WIDE) + u * WIDE, WIDE), WIDE)

    def row_unit(slot, j, u):
        return xg.at[slot, :, columns_of(j, u)]

    def row_half(ref, part):
        return ref.at[pl.ds(part * 80, 80 if part == 0 else ROWS - 80)]

    ag = Gather(p, row_unit, row_half, (g_zs, b_zr, g_xs, b_xr, g_ds, b_dr))
    for u in (1, 0):
        for jj in range(PLANE):
            here = jnp.logical_and(jj == p.j, 2 * p.j + u == p.exp)

            @pl.when(jnp.logical_not(here))
            def _(u=u, jj=jj):
                remote(rx.at[u, jj], rx.at[u, jj], x_s.at[0], x_r.at[u, jj], p.up).wait_recv()

        packed = jnp.dot(pack, rx[u].reshape(PLANE * PITCH, WIDE), preferred_element_type=F32)
        xg[0, :, columns_of(p.j, u)] = packed.astype(BF16)
        ag.start(u)
    for cp in weight_loads:
        cp.wait()
    ag.start_partner()

    def hidden(lo, hi):
        count = hi - lo
        rows = xg[lo:hi].reshape(count * ROWS, D)
        gate = lax.dot_general(rows, wg[...], (((1,), (1,)), ((), ())), preferred_element_type=F32)
        up = lax.dot_general(rows, wu[...], (((1,), (1,)), ((), ())), preferred_element_type=F32)
        act = gate / (1.0 + jnp.exp(-gate)) * up
        hb[lo:hi] = act.astype(BF16).reshape(count, ROWS, FF_LOCAL)

    def hidden_all(d):
        slots = slots_of(d, half)
        hidden(slots[0], slots[-1] + 1)

    sent = []

    def send(src, dst, ss, rs, device):
        cp = remote(src, dst, ss, rs, device)
        cp.start()
        sent.append(cp)

    def wait_for(ref, rs):
        remote(ref, ref, c_zs.at[0, 0], rs, p.up).wait_recv()

    def wide_columns(j):
        return pl.ds(pl.multiple_of(j * (2 * WIDE), 2 * WIDE), 2 * WIDE)

    def produce(slot):
        def part(n, _):
            cols = pl.ds(pl.multiple_of(n * WIDE, WIDE), WIDE)
            yb[slot, :, cols] = jnp.dot(hb[slot], wd[:, cols], preferred_element_type=F32).astype(BF16)
            return 0

        lax.fori_loop(0, D // WIDE, part, 0)
        for k, j in enumerate((p.jc, p.jcp)):
            send(yb.at[slot, :, wide_columns(j)], dr_buf.at[slot, k], c_ds.at[slot, k], c_dr.at[slot, k], p.sibling)

    def for_partner(slot):
        for k in range(2):
            wait_for(dr_buf.at[slot, k], c_dr.at[slot, k])
        cols = columns_of(p.jp, 1)
        yb[slot, :, cols] = (yb[slot, :, cols].astype(F32) + dr_buf[slot, 1, :, WIDE:].astype(F32)).astype(BF16)
        send(yb.at[slot, :, cols], xr_buf.at[slot], c_xs.at[slot], c_xr.at[slot], p.partner)

    def halves(ref, part):
        return ref.at[:, pl.ds(part * (WIDE // 2), WIDE // 2)]

    def reduce_unit(slot, d, k):
        for j, u in (((p.j, 0), (p.j, 1), (p.jp, 0))[k],):
            cols = columns_of(j, u)
            own = k != 2
            total = yb[slot, :, cols].astype(F32)
            total = total + dr_buf[slot, 0 if own else 1, :, pl.ds(u * WIDE, WIDE)].astype(F32)
            if k == 1:
                wait_for(xr_buf.at[slot], c_xr.at[slot])
                total = total + xr_buf[slot].astype(F32)
            if d == half:
                yb[slot, :, cols] = total.astype(BF16)
            elif d == half - 1:
                part = 0 if slot % 2 == 1 else 1
                wait_for(halves(zr_buf.at[slot, k], part), c_zr.at[slot, k])
                cut = slice(part * (WIDE // 2), (part + 1) * (WIDE // 2))
                keep = slice((1 - part) * (WIDE // 2), (2 - part) * (WIDE // 2))
                zr = zr_buf[slot, k, :, cut].astype(F32)
                base = j * (2 * WIDE) + u * WIDE
                for piece, value in ((cut, total[:, cut] + zr), (keep, total[:, keep])):
                    at = pl.ds(pl.multiple_of(base + piece.start, WIDE // 2), WIDE // 2)
                    yb[slot, :, at] = value.astype(BF16)
            else:
                sources = (0, 2 * half - 1) if slot == 0 else (slot,)
                for i in sources:
                    wait_for(zr_buf.at[i, k], c_zr.at[i, k])
                    total = total + zr_buf[i, k].astype(F32)
                yb[slot, :, cols] = total.astype(BF16)
            if d == 0:
                if k == 2:
                    send(yb.at[slot, :, cols], xr_buf.at[8], c_xs.at[8], c_xr.at[8], p.partner)
            elif d == half:
                for part in (0, 1):
                    to = 2 * (d - 1) - 1 + part
                    base = j * (2 * WIDE) + u * WIDE + part * (WIDE // 2)
                    send(
                        yb.at[slot, :, pl.ds(pl.multiple_of(base, WIDE // 2), WIDE // 2)],
                        halves(zr_buf.at[to, k], part),
                        c_zs.at[slot + part, k], c_zr.at[to, k], p.down if part == 0 else p.up,
                    )
            else:
                plus = slot % 2 == 1
                if d == 1:
                    to = 0 if plus else 2 * half - 1
                else:
                    to = slot - 2
                send(
                    yb.at[slot, :, cols], zr_buf.at[to, k], c_zs.at[slot, k], c_zr.at[to, k],
                    p.down if plus else p.up,
                )

    last, next_in = slots_of(half, half), slots_of(half - 1, half)
    for d in range(1, half + 1):
        near = slots_of(d - 1, half)

        def between(k):
            if k == 1:
                ag.arrive_partner(near)
            elif k == 0:
                ag.arrive_sibling(near)
                hidden_all(d - 1)

        ag.arrive(d, between)
    ag.arrive_partner(last)
    produce(next_in[0])
    ag.arrive_sibling(last)

    hidden_all(half)
    for s in last:
        produce(s)
    for_partner(next_in[0])
    for s in next_in[1:]:
        produce(s)
    for s in last:
        for_partner(s)
    for d in range(half, 0, -1):
        for k in (0, 2):
            for s in slots_of(d, half):
                reduce_unit(s, d, k)
        for s in slots_of(d - 1, half):
            if s != next_in[0]:
                for_partner(s)
        if d < half:
            for s in slots_of(d + 1, half):
                reduce_unit(s, d + 1, 1)
        if d > 1:
            for s in slots_of(d - 2, half):
                produce(s)

    r_sends = []

    def give_back(u):
        spread = lax.dot_general(pack, fb[u], (((0,), (0,)), ((), ())), preferred_element_type=F32)
        rb[u] = spread.astype(BF16).reshape(PLANE, PITCH, WIDE)
        for jj in range(PLANE):
            here = jnp.logical_and(jj == p.j, 2 * p.j + u == p.exp)
            cp = remote(rb.at[u, jj], ret.at[p.exp], r_s.at[u * PLANE + jj], r_r.at[p.exp], p.at(p.z, jj, 2 * p.j + u))
            r_sends.append((here, cp))
            pl.when(jnp.logical_not(here))(cp.start)

            @pl.when(here)
            def _():
                ret[p.exp] = rb[u, jj]

    reduce_unit(0, 0, 2)
    reduce_unit(0, 0, 0)
    for s in slots_of(1, half):
        reduce_unit(s, 1, 1)
    wait_for(xr_buf.at[8], c_xr.at[8])
    fb[0] = (yb[0, :, columns_of(p.j, 0)].astype(F32) + xr_buf[8].astype(F32)).astype(BF16)
    give_back(0)
    reduce_unit(0, 0, 1)
    fb[1] = yb[0, :, columns_of(p.j, 1)]
    give_back(1)

    ag.finish()
    for cp in sent:
        cp.wait_send()
    for cp in ss_sends:
        cp.wait_send()
    for i, cp in enumerate(x_sends):
        if i == 0:
            pl.when(jnp.logical_not(mine))(cp.wait_send)
        else:
            cp.wait_send()

    for i in range(n_exp):
        f = lax.rem(p.exp + i, n_exp)
        cp = remote(ret.at[f], ret.at[f], r_s.at[0], r_r.at[f], p.up)
        if i == 0:
            pl.when(jnp.logical_not(mine))(cp.wait_recv)
        else:
            cp.wait_recv()
    returned = ret[...].reshape(EXPERTS * PITCH, WIDE).astype(F32)
    mix_out[...] = lax.dot_general(
        mixed[...], returned, (((0,), (0,)), ((), ())), precision=lax.Precision.HIGHEST, preferred_element_type=F32
    )
    for here, cp in r_sends:
        pl.when(jnp.logical_not(here))(cp.wait_send)


def shards(depth, queries, keys, values, residual, norm_gain, routes, gates, w_gate, w_up, w_down):
    hbm_spec = pl.BlockSpec(memory_space=pltpu.HBM)
    vmem_spec = pl.BlockSpec(memory_space=pltpu.VMEM)
    slots = depth
    vmem, dma = pltpu.VMEM, pltpu.SemaphoreType.DMA
    tok_block = jax.ShapeDtypeStruct((TOK, WIDE), F32)
    scratch = [
        vmem((TOK, WIDE), BF16), vmem((TOK, WIDE), BF16), vmem((1, WIDE), F32), vmem((2, TOK), jnp.int32),
        vmem((2, TOK), F32), vmem((FF_LOCAL, D), BF16), vmem((FF_LOCAL, D), BF16), vmem((FF_LOCAL, D), BF16),
        vmem((slots, PLANE, 2, TOK, HEAD_WIDTH), BF16),
        vmem((GROUP * TOK, HEAD_WIDTH), BF16), vmem((GROUP * TOK, 1), F32), vmem((GROUP * TOK, 1), F32),
        vmem((GROUP * TOK, HEAD_WIDTH), F32), vmem((TOK, WIDE), BF16), vmem((EXPERTS, 8, 128), F32),
        vmem((EXPERTS, PITCH, WIDE), BF16), vmem((2, PLANE, PITCH, WIDE), BF16),
        vmem((slots, ROWS, D), BF16), vmem((slots, ROWS, FF_LOCAL), BF16), vmem((slots, ROWS, D), BF16),
        vmem((slots, 2, ROWS, 2 * WIDE), BF16), vmem((slots, 3, ROWS, WIDE), BF16), vmem((9, ROWS, WIDE), BF16),
        vmem((2, ROWS, WIDE), BF16), vmem((2, PLANE, PITCH, WIDE), BF16), vmem((EXPERTS, PITCH, WIDE), BF16),
        vmem((EXPERTS * PITCH, TOK), F32),
        dma((10,)),
        dma((9, 3)), dma((9,)), dma((8, 4)),
        dma((9, 2)), dma((1,)), dma((8, 2)),
        dma((9, 3)), dma((9,)), dma((8, 4)),
        dma((8,)), dma((8,)), dma((8,)), dma((2, PLANE)),
        dma((9, 3)), dma((9, 3)), dma((9,)), dma((9,)), dma((8, 2)), dma((8, 2)),
        dma((8,)), dma((8,)),
    ]
    attn, mix = pl.pallas_call(
        functools.partial(kernel, depth),
        out_shape=(tok_block, tok_block),
        in_specs=[hbm_spec] * 10,
        out_specs=(vmem_spec, vmem_spec),
        scratch_shapes=scratch,
        compiler_params=pltpu.CompilerParams(
            collective_id=0, has_side_effects=True, vmem_limit_bytes=VMEM_BYTES
        ),
    )(
        queries, keys, values, residual, norm_gain.reshape(1, WIDE), routes.T, gates.T,
        w_gate[0].T, w_up[0].T, w_down[0],
    )
    attended = lax.reduce_precision(residual.astype(F32) + attn, 8, 7)
    return attended.astype(BF16), (attended + mix).astype(BF16)


def solution(mesh):
    in_specs = (
        P("seq", "exp"), P("seq", "exp"), P("seq", "exp"), P("seq", "exp"), P("exp"), P("seq", None), P("seq", None),
        P("exp", None, "seq"), P("exp", None, "seq"), P("exp", "seq", None),
    )
    body = functools.partial(shards, mesh.shape["seq"] // PLANE)
    return jax.shard_map(body, mesh=mesh, in_specs=in_specs, out_specs=(P("seq", "exp"), P("seq", "exp")), check_vma=False)
```

```python
import functools
import math

import jax
import jax.numpy as jnp
from jax import lax
from jax.experimental import pallas as pl
from jax.experimental.pallas import tpu as pltpu
from jax.sharding import PartitionSpec as P

D = 4096
HEAD_WIDTH = 128
GROUP = 4
TOK = 96
EXPERTS = 8
CAP = 36
PITCH = 40
PLANE = 4
ROWS = PLANE * CAP
WIDE = 512
FF_LOCAL = 448
MESH = pl.DeviceIdType.MESH
VMEM_BYTES = 63 * 1024 * 1024
F32 = jnp.float32
BF16 = jnp.bfloat16


class Place:
    def __init__(self, depth):
        self.depth = depth
        self.half = depth // 2
        self.seq = lax.axis_index("seq")
        self.exp = lax.axis_index("exp")
        self.z = self.seq // PLANE
        self.j = lax.rem(self.seq, PLANE)
        xh, c = self.j // 2, lax.rem(self.j, 2)
        self.jp = (1 - xh) * 2 + c
        self.jc = xh * 2 + (1 - c)
        self.jcp = (1 - xh) * 2 + (1 - c)
        self.up = self.at(lax.rem(self.z + 1, depth), self.j)
        self.down = self.at(lax.rem(self.z + depth - 1, depth), self.j)
        self.up_other = self.at(lax.rem(self.z + 1, depth), self.jp)
        self.down_other = self.at(lax.rem(self.z + depth - 1, depth), self.jp)
        self.partner = self.at(self.z, self.jp)
        self.sibling = self.at(self.z, self.jc)

    def at(self, z, j, e=None):
        return {"seq": z * PLANE + j, "exp": self.exp if e is None else e}


def remote(src, dst, send_sem, recv_sem, device):
    return pltpu.make_async_remote_copy(
        src_ref=src, dst_ref=dst, send_sem=send_sem, recv_sem=recv_sem,
        device_id=device, device_id_type=MESH,
    )


class Gather:
    def __init__(self, place, unit, half, sems):
        self.p, self.unit, self.cut = place, unit, half
        self.zs, self.zr, self.xs, self.xr, self.ds, self.dr = sems
        self.sent = []

    def send(self, ref, ss, rs, device):
        cp = remote(ref, ref, ss, rs, device)
        cp.start()
        self.sent.append(cp)

    def got(self, ref, rs):
        remote(ref, ref, self.zs.at[0, 0], rs, self.p.up).wait_recv()

    def ring(self, src_slot, plus, d, k, j, u):
        h = self.p.half
        sem = 2 * (d + 1) - 1 if plus else 2 * (d + 1)
        dst_slot = min(sem, 2 * h - 1)
        src, dst = self.unit(src_slot, j, u), self.unit(dst_slot, j, u)
        if d + 1 == h:
            src, dst = self.cut(src, 0 if plus else 1), self.cut(dst, 0 if plus else 1)
        cp = remote(src, dst, self.zs.at[sem, k], self.zr.at[sem, k], self.p.up if plus else self.p.down)
        cp.start()
        self.sent.append(cp)

    def across(self, slot, k, j, u):
        self.send(self.unit(slot, j, u), self.ds.at[slot, k], self.dr.at[slot, k], self.p.sibling)

    def start(self, u):
        p = self.p
        if u == 0:
            self.send(self.unit(0, p.j, 0), self.xs.at[8], self.xr.at[8], p.partner)
        self.ring(0, True, 0, u, p.j, u)
        self.ring(0, False, 0, u, p.j, u)
        self.across(0, u, p.j, u)
        if u == 0:
            self.send(self.unit(0, p.j, 1), self.xs.at[0], self.xr.at[0], p.partner)

    def start_partner(self):
        p = self.p
        self.got(self.unit(0, p.jp, 0), self.xr.at[8])
        self.ring(0, True, 0, 2, p.jp, 0)
        self.ring(0, False, 0, 2, p.jp, 0)
        self.across(0, 2, p.jp, 0)

    def arrive(self, d, after):
        p, h = self.p, self.p.half
        for k, own, u in ((1, True, 1), (0, True, 0), (2, False, 0)):
            j = p.j if own else p.jp
            if d < h:
                for plus in (True, False):
                    slot = 2 * d - 1 if plus else 2 * d
                    self.got(self.unit(slot, j, u), self.zr.at[slot, k])
                    self.ring(slot, plus, d, k, j, u)
                slots = (2 * d - 1, 2 * d)
            else:
                slot = 2 * h - 1
                for part in (0, 1):
                    self.got(self.cut(self.unit(slot, j, u), part), self.zr.at[slot + part, k])
                slots = (slot,)
            for slot in slots:
                if k == 1:
                    self.send(self.unit(slot, j, 1), self.xs.at[slot], self.xr.at[slot], p.partner)
                self.across(slot, k, j, u)
            after(k)

    def arrive_partner(self, slots):
        for slot in slots:
            self.got(self.unit(slot, self.p.jp, 1), self.xr.at[slot])
            self.across(slot, 3, self.p.jp, 1)

    def arrive_sibling(self, slots):
        p = self.p
        for slot in slots:
            for k, (j, u) in enumerate(((p.jc, 0), (p.jc, 1), (p.jcp, 0), (p.jcp, 1))):
                self.got(self.unit(slot, j, u), self.dr.at[slot, k])

    def finish(self):
        for cp in self.sent:
            cp.wait_send()


class KvGather:
    def __init__(self, place, kv, sems):
        self.p, self.kv = place, kv
        self.zs, self.zr, self.xs, self.xr, self.ds, self.dr = sems
        self.sent = []

    def send(self, ref, ss, rs, device):
        cp = remote(ref, ref, ss, rs, device)
        cp.start()
        self.sent.append(cp)

    def got(self, ref, rs):
        remote(ref, ref, self.zs.at[0, 0], rs, self.p.up).wait_recv()

    def ring(self, src_slot, plus, d, k):
        p, h = self.p, self.p.half
        sem = 2 * (d + 1) - 1 if plus else 2 * (d + 1)
        src, dst = self.kv.at[src_slot, p.j], self.kv.at[min(sem, 2 * h - 1), p.j]
        if d + 1 == h:
            part = 0 if plus else 1
            src, dst = src.at[part], dst.at[part]
        device = ((p.up, p.up_other) if plus else (p.down, p.down_other))[k]
        cp = remote(src, dst, self.zs.at[sem, k], self.zr.at[sem, k], device)
        cp.start()
        self.sent.append(cp)

    def across(self, slot, k, j):
        self.send(self.kv.at[slot, j], self.ds.at[slot, k], self.dr.at[slot, k], self.p.sibling)

    def start(self):
        p = self.p
        for k in (0, 1):
            self.ring(0, True, 0, k)
            self.ring(0, False, 0, k)
        self.send(self.kv.at[0, p.j], self.xs.at[0], self.xr.at[0], p.partner)
        self.across(0, 0, p.j)

    def arrive(self, d):
        p, h = self.p, self.p.half
        for slot in slots_of(d, h):
            if d < h:
                self.got(self.kv.at[slot, p.j], self.zr.at[slot, 0])
                for k in (0, 1):
                    self.ring(slot, slot % 2 == 1, d, k)
            else:
                for part in (0, 1):
                    self.got(self.kv.at[slot, p.j, part], self.zr.at[slot + part, 0])
            self.across(slot, 0, p.j)

    def arrive_other(self, d):
        p, h = self.p, self.p.half
        for slot in slots_of(d, h):
            if d == 0:
                self.got(self.kv.at[slot, p.jp], self.xr.at[0])
            elif d < h:
                self.got(self.kv.at[slot, p.jp], self.zr.at[slot, 1])
            else:
                for part in (0, 1):
                    self.got(self.kv.at[slot, p.jp, part], self.zr.at[slot + part, 1])
            self.across(slot, 1, p.jp)

    def arrive_sibling(self, slots):
        p = self.p
        for slot in slots:
            for k, j in enumerate((p.jc, p.jcp)):
                self.got(self.kv.at[slot, j], self.dr.at[slot, k])

    def finish(self):
        for cp in self.sent:
            cp.wait_send()


def slots_of(d, half):
    if d == 0:
        return (0,)
    return (2 * d - 1, 2 * d) if d < half else (2 * half - 1,)


def kernel(
    depth,
    q_hbm, k_hbm, v_hbm, res_hbm, gain_hbm, routes_hbm, gates_hbm, wg_hbm, wu_hbm, wd_hbm,
    attn_out, mix_out,
    q_in, res_in, gain_in, routes_in, gates_in, wg, wu, wd,
    kvg, qs, m_s, l_s, acc_s, att, ss_buf, outgoing, rx, xg, hb, yb, dr_buf, zr_buf, xr_buf, fb, rb, ret, mixed, placed, roots,
    load_sem, g_zs, g_xs, g_ds, a_zr, a_xr, a_dr, b_zr, b_xr, b_dr,
    i_zs, i_zr, i_xs, i_xr, i_ds, i_dr, ss_s, ss_r, x_s, x_r, c_zs, c_zr, c_xs, c_xr, c_ds, c_dr, r_s, r_r,
):
    p = Place(depth)
    half = p.half
    n_exp = EXPERTS

    def load(src, dst, i):
        cp = pltpu.make_async_copy(src, dst, load_sem.at[i])
        cp.start()
        return cp

    loads = [
        load(k_hbm, kvg.at[0, p.j, 0], 0), load(v_hbm, kvg.at[0, p.j, 1], 1), load(q_hbm, q_in, 2),
        load(res_hbm, res_in, 3), load(gain_hbm, gain_in, 4), load(routes_hbm, routes_in, 5),
        load(gates_hbm, gates_in, 6),
    ]

    barrier = pltpu.get_barrier_semaphore()

    def greet(device):
        pl.semaphore_signal(barrier, inc=1, device_id=device, device_id_type=MESH)

    for device in (p.up, p.down, p.up_other, p.down_other, p.partner, p.sibling):
        greet(device)
    for i in range(1, n_exp):
        greet(p.at(p.z, p.j, lax.rem(p.exp + i, n_exp)))
    home = p.exp // 2
    mine = home == p.j
    for i in range(n_exp):
        f = lax.rem(p.exp + i, n_exp)
        if i == 0:
            @pl.when(jnp.logical_not(mine))
            def _():
                greet(p.at(p.z, home, f))
        else:
            greet(p.at(p.z, home, f))
    for u in range(2):
        for jj in range(PLANE):
            src_e = 2 * p.j + u

            @pl.when(jnp.logical_not(jnp.logical_and(jj == p.j, src_e == p.exp)))
            def _():
                greet(p.at(p.z, jj, src_e))
    pl.semaphore_wait(barrier, 6 + (n_exp - 1) + 16 - 2 * mine.astype(jnp.int32))

    loads[0].wait()
    loads[1].wait()

    kv = KvGather(p, kvg, (g_zs, a_zr, g_xs, a_xr, g_ds, a_dr))
    kv.start()

    weight_loads = [load(wg_hbm, wg, 7), load(wu_hbm, wu, 8), load(wd_hbm, wd, 9)]
    for cp in loads[2:]:
        cp.wait()

    for h in range(GROUP):
        qs[pl.ds(h * TOK, TOK), :] = q_in[:, h * HEAD_WIDTH:(h + 1) * HEAD_WIDTH]

    r_row = [routes_in[k:k + 1, :] for k in range(2)]
    expert_ids = lax.broadcasted_iota(jnp.int32, (EXPERTS, TOK), 0)
    one_hot = [(expert_ids == r_row[k]).astype(F32) for k in range(2)]
    earlier = (
        lax.broadcasted_iota(jnp.int32, (TOK, TOK), 0) < lax.broadcasted_iota(jnp.int32, (TOK, TOK), 1)
    ).astype(BF16)
    before = jnp.dot((one_hot[0] + one_hot[1]).astype(BF16), earlier, preferred_element_type=F32)
    slot_row = [jnp.sum(one_hot[k] * before, axis=0, keepdims=True) for k in range(2)]
    dest = [r_row[k] * PITCH + slot_row[k].astype(jnp.int32) for k in range(2)]
    slot_ids = lax.broadcasted_iota(jnp.int32, (EXPERTS * PITCH, TOK), 0)
    match = [slot_ids == dest[k] for k in range(2)]
    dispatch = jnp.where(jnp.logical_or(match[0], match[1]), 1.0, 0.0).astype(F32)
    placed[...] = dispatch
    mixed[...] = jnp.where(match[0], gates_in[0:1, :], 0.0) + jnp.where(match[1], gates_in[1:2, :], 0.0)

    scale = 1.0 / math.sqrt(HEAD_WIDTH)
    kv_rows = PLANE * TOK

    def attend(slot, first):
        keys = kvg[slot, :, 0].reshape(kv_rows, HEAD_WIDTH)
        vals = kvg[slot, :, 1].reshape(kv_rows, HEAD_WIDTH)
        scores = lax.dot_general(qs[...], keys, (((1,), (1,)), ((), ())), preferred_element_type=F32) * scale
        if first:
            at = lax.broadcasted_iota(jnp.int32, scores.shape, 0)
            for h in range(1, GROUP):
                at = at - jnp.where(lax.broadcasted_iota(jnp.int32, scores.shape, 0) >= h * TOK, TOK, 0)
            seen = lax.broadcasted_iota(jnp.int32, scores.shape, 1) <= at + p.j * TOK
            scores = jnp.where(seen, scores, -1e30)
            top = jnp.max(scores, axis=1, keepdims=True)
            terms = jnp.where(seen, jnp.exp(scores - top), 0.0)
            m_s[...] = top
            l_s[...] = jnp.sum(terms, axis=1, keepdims=True)
            acc_s[...] = jnp.dot(terms.astype(BF16), vals, preferred_element_type=F32)
        else:
            old = m_s[...]
            top = jnp.maximum(old, jnp.max(scores, axis=1, keepdims=True))
            fade = jnp.exp(old - top)
            terms = jnp.exp(scores - top)
            m_s[...] = top
            l_s[...] = l_s[...] * fade + jnp.sum(terms, axis=1, keepdims=True)
            acc_s[...] = acc_s[...] * fade + jnp.dot(terms.astype(BF16), vals, preferred_element_type=F32)

    def attend_all(d):
        for slot in slots_of(d, half):
            if slot == 0:
                attend(0, True)
            else:
                if d == half:
                    seen = p.z >= half
                elif slot % 2 == 1:
                    seen = p.z >= d
                else:
                    seen = p.z + d >= depth

                @pl.when(seen)
                def _(slot=slot):
                    attend(slot, False)

    for d in range(1, half + 1):
        kv.arrive(d)
        kv.arrive_other(d - 1)
        kv.arrive_sibling(slots_of(d - 1, half))
        attend_all(d - 1)
    kv.arrive_other(half)
    kv.arrive_sibling(slots_of(half, half))
    attend_all(half)

    for h in range(GROUP):
        rows, cols = slice(h * TOK, (h + 1) * TOK), slice(h * HEAD_WIDTH, (h + 1) * HEAD_WIDTH)
        attn = acc_s[rows, :] / l_s[rows, :]
        attn_out[:, cols] = attn
        att[:, cols] = (res_in[:, cols].astype(F32) + attn).astype(BF16)

    stream = att[...].astype(F32)
    squares = lax.dot_general(
        jnp.ones((8, WIDE), F32), stream * stream, (((1,), (1,)), ((), ())),
        precision=lax.Precision.HIGHEST, preferred_element_type=F32,
    )
    ss_buf[p.exp, :, pl.ds(0, TOK)] = squares
    ss_sends = []
    for i in range(1, n_exp):
        other = lax.rem(p.exp + i, n_exp)
        cp = remote(ss_buf.at[p.exp], ss_buf.at[p.exp], ss_s.at[i], ss_r.at[i], p.at(p.z, p.j, other))
        cp.start()
        ss_sends.append(cp)
    rows_out = jnp.dot(dispatch.astype(BF16), att[...], preferred_element_type=F32)
    outgoing[...] = (rows_out * gain_in[...]).astype(BF16).reshape(EXPERTS, PITCH, WIDE)

    u_me = lax.rem(p.exp, 2)
    x_sends = []
    for i in range(n_exp):
        f = lax.rem(p.exp + i, n_exp)
        cp = remote(outgoing.at[f], rx.at[u_me, p.j], x_s.at[i], x_r.at[u_me, p.j], p.at(p.z, home, f))
        x_sends.append(cp)
        if i == 0:
            pl.when(jnp.logical_not(mine))(cp.start)

            @pl.when(mine)
            def _():
                rx[u_me, p.j] = outgoing[p.exp]
        else:
            cp.start()

    kv.finish()

    for i in range(1, n_exp):
        other = lax.rem(p.exp + n_exp - i, n_exp)
        remote(ss_buf.at[other], ss_buf.at[other], ss_s.at[i], ss_r.at[i], p.up).wait_recv()
    total = ss_buf[0, :, pl.ds(0, TOK)]
    for i in range(1, n_exp):
        total = total + ss_buf[i, :, pl.ds(0, TOK)]
    inverse = lax.rsqrt(total / D + 1e-05)

    own_rows = placed[pl.ds(pl.multiple_of(p.exp * PITCH, PITCH), PITCH), :]
    roots[0, p.j] = jnp.zeros((2, 8, 128), F32)
    inverse_of = lax.dot_general(
        inverse, own_rows, (((1,), (1,)), ((), ())), precision=lax.Precision.HIGHEST, preferred_element_type=F32
    )
    for part in range(2):
        roots[0, p.j, part, :, pl.ds(0, PITCH)] = inverse_of
    iv = KvGather(p, roots, (i_zs, i_zr, i_xs, i_xr, i_ds, i_dr))
    iv.start()

    iv.arrive(1)

    row_ids = lax.broadcasted_iota(jnp.int32, (ROWS, PLANE * PITCH), 0)
    for i in range(1, PLANE):
        row_ids = row_ids + jnp.where(
            lax.broadcasted_iota(jnp.int32, (ROWS, PLANE * PITCH), 0) >= i * CAP, PITCH - CAP, 0
        )
    pack = (row_ids == lax.broadcasted_iota(jnp.int32, (ROWS, PLANE * PITCH), 1)).astype(BF16)

    def columns_of(j, u):
        return pl.ds(pl.multiple_of(j * (2 * WIDE) + u * WIDE, WIDE), WIDE)

    def row_unit(slot, j, u):
        return xg.at[slot, :, columns_of(j, u)]

    def row_half(ref, part):
        return ref.at[pl.ds(part * 80, 80 if part == 0 else ROWS - 80)]

    ag = Gather(p, row_unit, row_half, (g_zs, b_zr, g_xs, b_xr, g_ds, b_dr))
    for u in (1, 0):
        for jj in range(PLANE):
            here = jnp.logical_and(jj == p.j, 2 * p.j + u == p.exp)

            @pl.when(jnp.logical_not(here))
            def _(u=u, jj=jj):
                remote(rx.at[u, jj], rx.at[u, jj], x_s.at[0], x_r.at[u, jj], p.up).wait_recv()

        packed = jnp.dot(pack, rx[u].reshape(PLANE * PITCH, WIDE), preferred_element_type=F32)
        xg[0, :, columns_of(p.j, u)] = packed.astype(BF16)
        ag.start(u)
    for cp in weight_loads:
        cp.wait()
    ag.start_partner()
    iv.arrive(2)

    lane_ids = lax.broadcasted_iota(jnp.int32, (ROWS, 128), 1)
    line_ids = lax.broadcasted_iota(jnp.int32, (ROWS, 128), 0)

    def roots_of(slot):
        spread = jnp.zeros((ROWS, 128), F32)
        for jj in range(PLANE):
            at = jnp.logical_and(line_ids - jj * CAP == lane_ids, lane_ids < CAP)
            spread = spread + jnp.where(at, roots[slot, jj, 0, 0:1, :], 0.0)
        return jnp.sum(spread, axis=1, keepdims=True)

    def hidden(lo, hi):
        count = hi - lo
        root = jnp.concatenate([roots_of(slot) for slot in range(lo, hi)], axis=0)
        rows = xg[lo:hi].reshape(count * ROWS, D)
        gate = lax.dot_general(rows, wg[...], (((1,), (1,)), ((), ())), preferred_element_type=F32)
        up = lax.dot_general(rows, wu[...], (((1,), (1,)), ((), ())), preferred_element_type=F32)
        gate, up = gate * root, up * root
        act = gate / (1.0 + jnp.exp(-gate)) * up
        hb[lo:hi] = act.astype(BF16).reshape(count, ROWS, FF_LOCAL)

    def hidden_all(d):
        slots = slots_of(d, half)
        iv.arrive_other(d)
        iv.arrive_sibling(slots)
        hidden(slots[0], slots[-1] + 1)

    sent = []

    def send(src, dst, ss, rs, device):
        cp = remote(src, dst, ss, rs, device)
        cp.start()
        sent.append(cp)

    def wait_for(ref, rs):
        remote(ref, ref, c_zs.at[0, 0], rs, p.up).wait_recv()

    def wide_columns(j):
        return pl.ds(pl.multiple_of(j * (2 * WIDE), 2 * WIDE), 2 * WIDE)

    def produce(slot):
        def part(n, _):
            cols = pl.ds(pl.multiple_of(n * WIDE, WIDE), WIDE)
            yb[slot, :, cols] = jnp.dot(hb[slot], wd[:, cols], preferred_element_type=F32).astype(BF16)
            return 0

        lax.fori_loop(0, D // WIDE, part, 0)
        for k, j in enumerate((p.jc, p.jcp)):
            send(yb.at[slot, :, wide_columns(j)], dr_buf.at[slot, k], c_ds.at[slot, k], c_dr.at[slot, k], p.sibling)

    def for_partner(slot):
        for k in range(2):
            wait_for(dr_buf.at[slot, k], c_dr.at[slot, k])
        cols = columns_of(p.jp, 1)
        yb[slot, :, cols] = (yb[slot, :, cols].astype(F32) + dr_buf[slot, 1, :, WIDE:].astype(F32)).astype(BF16)
        send(yb.at[slot, :, cols], xr_buf.at[slot], c_xs.at[slot], c_xr.at[slot], p.partner)

    def halves(ref, part):
        return ref.at[:, pl.ds(part * (WIDE // 2), WIDE // 2)]

    def reduce_unit(slot, d, k):
        for j, u in (((p.j, 0), (p.j, 1), (p.jp, 0))[k],):
            cols = columns_of(j, u)
            own = k != 2
            total = yb[slot, :, cols].astype(F32)
            total = total + dr_buf[slot, 0 if own else 1, :, pl.ds(u * WIDE, WIDE)].astype(F32)
            if k == 1:
                wait_for(xr_buf.at[slot], c_xr.at[slot])
                total = total + xr_buf[slot].astype(F32)
            if d == half:
                yb[slot, :, cols] = total.astype(BF16)
            elif d == half - 1:
                part = 0 if slot % 2 == 1 else 1
                wait_for(halves(zr_buf.at[slot, k], part), c_zr.at[slot, k])
                cut = slice(part * (WIDE // 2), (part + 1) * (WIDE // 2))
                keep = slice((1 - part) * (WIDE // 2), (2 - part) * (WIDE // 2))
                zr = zr_buf[slot, k, :, cut].astype(F32)
                base = j * (2 * WIDE) + u * WIDE
                for piece, value in ((cut, total[:, cut] + zr), (keep, total[:, keep])):
                    at = pl.ds(pl.multiple_of(base + piece.start, WIDE // 2), WIDE // 2)
                    yb[slot, :, at] = value.astype(BF16)
            else:
                sources = (0, 2 * half - 1) if slot == 0 else (slot,)
                for i in sources:
                    wait_for(zr_buf.at[i, k], c_zr.at[i, k])
                    total = total + zr_buf[i, k].astype(F32)
                yb[slot, :, cols] = total.astype(BF16)
            if d == 0:
                if k == 2:
                    send(yb.at[slot, :, cols], xr_buf.at[8], c_xs.at[8], c_xr.at[8], p.partner)
            elif d == half:
                for part in (0, 1):
                    to = 2 * (d - 1) - 1 + part
                    base = j * (2 * WIDE) + u * WIDE + part * (WIDE // 2)
                    send(
                        yb.at[slot, :, pl.ds(pl.multiple_of(base, WIDE // 2), WIDE // 2)],
                        halves(zr_buf.at[to, k], part),
                        c_zs.at[slot + part, k], c_zr.at[to, k], p.down if part == 0 else p.up,
                    )
            else:
                plus = slot % 2 == 1
                if d == 1:
                    to = 0 if plus else 2 * half - 1
                else:
                    to = slot - 2
                send(
                    yb.at[slot, :, cols], zr_buf.at[to, k], c_zs.at[slot, k], c_zr.at[to, k],
                    p.down if plus else p.up,
                )

    last, next_in = slots_of(half, half), slots_of(half - 1, half)
    for d in range(1, half + 1):
        near = slots_of(d - 1, half)

        def between(k):
            if k == 1:
                ag.arrive_partner(near)
            elif k == 0:
                ag.arrive_sibling(near)
                hidden_all(d - 1)
            elif d + 2 <= half:
                iv.arrive(d + 2)

        ag.arrive(d, between)
    ag.arrive_partner(last)
    produce(next_in[0])
    ag.arrive_sibling(last)

    hidden_all(half)
    for s in last:
        produce(s)
    for_partner(next_in[0])
    for s in next_in[1:]:
        produce(s)
    for s in last:
        for_partner(s)
    for d in range(half, 0, -1):
        for k in (0, 2):
            for s in slots_of(d, half):
                reduce_unit(s, d, k)
        for s in slots_of(d - 1, half):
            if s != next_in[0]:
                for_partner(s)
        if d < half:
            for s in slots_of(d + 1, half):
                reduce_unit(s, d + 1, 1)
        if d > 1:
            for s in slots_of(d - 2, half):
                produce(s)

    r_sends = []

    def give_back(u):
        spread = lax.dot_general(pack, fb[u], (((0,), (0,)), ((), ())), preferred_element_type=F32)
        rb[u] = spread.astype(BF16).reshape(PLANE, PITCH, WIDE)
        for jj in range(PLANE):
            here = jnp.logical_and(jj == p.j, 2 * p.j + u == p.exp)
            cp = remote(rb.at[u, jj], ret.at[p.exp], r_s.at[u * PLANE + jj], r_r.at[p.exp], p.at(p.z, jj, 2 * p.j + u))
            r_sends.append((here, cp))
            pl.when(jnp.logical_not(here))(cp.start)

            @pl.when(here)
            def _():
                ret[p.exp] = rb[u, jj]

    reduce_unit(0, 0, 2)
    reduce_unit(0, 0, 0)
    for s in slots_of(1, half):
        reduce_unit(s, 1, 1)
    wait_for(xr_buf.at[8], c_xr.at[8])
    fb[0] = (yb[0, :, columns_of(p.j, 0)].astype(F32) + xr_buf[8].astype(F32)).astype(BF16)
    give_back(0)
    reduce_unit(0, 0, 1)
    fb[1] = yb[0, :, columns_of(p.j, 1)]
    give_back(1)

    ag.finish()
    iv.finish()
    for cp in sent:
        cp.wait_send()
    for cp in ss_sends:
        cp.wait_send()
    for i, cp in enumerate(x_sends):
        if i == 0:
            pl.when(jnp.logical_not(mine))(cp.wait_send)
        else:
            cp.wait_send()

    for i in range(n_exp):
        f = lax.rem(p.exp + i, n_exp)
        cp = remote(ret.at[f], ret.at[f], r_s.at[0], r_r.at[f], p.up)
        if i == 0:
            pl.when(jnp.logical_not(mine))(cp.wait_recv)
        else:
            cp.wait_recv()
    returned = ret[...].reshape(EXPERTS * PITCH, WIDE).astype(F32)
    mix_out[...] = lax.dot_general(
        mixed[...], returned, (((0,), (0,)), ((), ())), precision=lax.Precision.HIGHEST, preferred_element_type=F32
    )
    for here, cp in r_sends:
        pl.when(jnp.logical_not(here))(cp.wait_send)


def shards(depth, queries, keys, values, residual, norm_gain, routes, gates, w_gate, w_up, w_down):
    hbm_spec = pl.BlockSpec(memory_space=pltpu.HBM)
    vmem_spec = pl.BlockSpec(memory_space=pltpu.VMEM)
    slots = depth
    vmem, dma = pltpu.VMEM, pltpu.SemaphoreType.DMA
    tok_block = jax.ShapeDtypeStruct((TOK, WIDE), F32)
    scratch = [
        vmem((TOK, WIDE), BF16), vmem((TOK, WIDE), BF16), vmem((1, WIDE), F32), vmem((2, TOK), jnp.int32),
        vmem((2, TOK), F32), vmem((FF_LOCAL, D), BF16), vmem((FF_LOCAL, D), BF16), vmem((FF_LOCAL, D), BF16),
        vmem((slots, PLANE, 2, TOK, HEAD_WIDTH), BF16),
        vmem((GROUP * TOK, HEAD_WIDTH), BF16), vmem((GROUP * TOK, 1), F32), vmem((GROUP * TOK, 1), F32),
        vmem((GROUP * TOK, HEAD_WIDTH), F32), vmem((TOK, WIDE), BF16), vmem((EXPERTS, 8, 128), F32),
        vmem((EXPERTS, PITCH, WIDE), BF16), vmem((2, PLANE, PITCH, WIDE), BF16),
        vmem((slots, ROWS, D), BF16), vmem((slots, ROWS, FF_LOCAL), BF16), vmem((slots, ROWS, D), BF16),
        vmem((slots, 2, ROWS, 2 * WIDE), BF16), vmem((slots, 3, ROWS, WIDE), BF16), vmem((9, ROWS, WIDE), BF16),
        vmem((2, ROWS, WIDE), BF16), vmem((2, PLANE, PITCH, WIDE), BF16), vmem((EXPERTS, PITCH, WIDE), BF16),
        vmem((EXPERTS * PITCH, TOK), F32), vmem((EXPERTS * PITCH, TOK), F32), vmem((slots, PLANE, 2, 8, 128), F32),
        dma((10,)),
        dma((9, 3)), dma((9,)), dma((8, 4)),
        dma((9, 2)), dma((1,)), dma((8, 2)),
        dma((9, 3)), dma((9,)), dma((8, 4)),
        dma((9, 2)), dma((9, 2)), dma((1,)), dma((1,)), dma((8, 2)), dma((8, 2)),
        dma((8,)), dma((8,)), dma((8,)), dma((2, PLANE)),
        dma((9, 3)), dma((9, 3)), dma((9,)), dma((9,)), dma((8, 2)), dma((8, 2)),
        dma((8,)), dma((8,)),
    ]
    attn, mix = pl.pallas_call(
        functools.partial(kernel, depth),
        out_shape=(tok_block, tok_block),
        in_specs=[hbm_spec] * 10,
        out_specs=(vmem_spec, vmem_spec),
        scratch_shapes=scratch,
        compiler_params=pltpu.CompilerParams(
            collective_id=0, has_side_effects=True, vmem_limit_bytes=VMEM_BYTES
        ),
    )(
        queries, keys, values, residual, norm_gain.reshape(1, WIDE), routes.T, gates.T,
        w_gate[0].T, w_up[0].T, w_down[0],
    )
    attended = lax.reduce_precision(residual.astype(F32) + attn, 8, 7)
    return attended.astype(BF16), (attended + mix).astype(BF16)


def solution(mesh):
    in_specs = (
        P("seq", "exp"), P("seq", "exp"), P("seq", "exp"), P("seq", "exp"), P("exp"), P("seq", None), P("seq", None),
        P("exp", None, "seq"), P("exp", None, "seq"), P("exp", "seq", None),
    )
    body = functools.partial(shards, mesh.shape["seq"] // PLANE)
    return jax.shard_map(body, mesh=mesh, in_specs=in_specs, out_specs=(P("seq", "exp"), P("seq", "exp")), check_vma=False)
```

```python
import functools
import math

import jax
import jax.numpy as jnp
from jax import lax
from jax.experimental import pallas as pl
from jax.experimental.pallas import tpu as pltpu
from jax.sharding import PartitionSpec as P

D = 4096
HEAD_WIDTH = 128
GROUP = 4
TOK = 96
EXPERTS = 8
CAP = 36
PITCH = 40
PLANE = 4
ROWS = PLANE * CAP
WIDE = 512
FF_LOCAL = 448
MESH = pl.DeviceIdType.MESH
VMEM_BYTES = 63 * 1024 * 1024
F32 = jnp.float32
BF16 = jnp.bfloat16


class Place:
    def __init__(self, depth):
        self.depth = depth
        self.half = depth // 2
        self.seq = lax.axis_index("seq")
        self.exp = lax.axis_index("exp")
        self.z = self.seq // PLANE
        self.j = lax.rem(self.seq, PLANE)
        xh, c = self.j // 2, lax.rem(self.j, 2)
        self.jp = (1 - xh) * 2 + c
        self.jc = xh * 2 + (1 - c)
        self.jcp = (1 - xh) * 2 + (1 - c)
        self.up = self.at(lax.rem(self.z + 1, depth), self.j)
        self.down = self.at(lax.rem(self.z + depth - 1, depth), self.j)
        self.up_other = self.at(lax.rem(self.z + 1, depth), self.jp)
        self.down_other = self.at(lax.rem(self.z + depth - 1, depth), self.jp)
        self.partner = self.at(self.z, self.jp)
        self.sibling = self.at(self.z, self.jc)

    def at(self, z, j, e=None):
        return {"seq": z * PLANE + j, "exp": self.exp if e is None else e}


def remote(src, dst, send_sem, recv_sem, device):
    return pltpu.make_async_remote_copy(
        src_ref=src, dst_ref=dst, send_sem=send_sem, recv_sem=recv_sem,
        device_id=device, device_id_type=MESH,
    )


class Gather:
    def __init__(self, place, unit, half, sems):
        self.p, self.unit, self.cut = place, unit, half
        self.zs, self.zr, self.xs, self.xr, self.ds, self.dr = sems
        self.sent = []

    def send(self, ref, ss, rs, device):
        cp = remote(ref, ref, ss, rs, device)
        cp.start()
        self.sent.append(cp)

    def got(self, ref, rs):
        remote(ref, ref, self.zs.at[0, 0], rs, self.p.up).wait_recv()

    def ring(self, src_slot, plus, d, k, j, u):
        h = self.p.half
        sem = 2 * (d + 1) - 1 if plus else 2 * (d + 1)
        dst_slot = min(sem, 2 * h - 1)
        src, dst = self.unit(src_slot, j, u), self.unit(dst_slot, j, u)
        if d + 1 == h:
            src, dst = self.cut(src, 0 if plus else 1), self.cut(dst, 0 if plus else 1)
        cp = remote(src, dst, self.zs.at[sem, k], self.zr.at[sem, k], self.p.up if plus else self.p.down)
        cp.start()
        self.sent.append(cp)

    def across(self, slot, k, j, u):
        self.send(self.unit(slot, j, u), self.ds.at[slot, k], self.dr.at[slot, k], self.p.sibling)

    def start(self, u):
        p = self.p
        if u == 0:
            self.send(self.unit(0, p.j, 0), self.xs.at[8], self.xr.at[8], p.partner)
        self.ring(0, True, 0, u, p.j, u)
        self.ring(0, False, 0, u, p.j, u)
        self.across(0, u, p.j, u)
        if u == 0:
            self.send(self.unit(0, p.j, 1), self.xs.at[0], self.xr.at[0], p.partner)

    def start_partner(self):
        p = self.p
        self.got(self.unit(0, p.jp, 0), self.xr.at[8])
        self.ring(0, True, 0, 2, p.jp, 0)
        self.ring(0, False, 0, 2, p.jp, 0)
        self.across(0, 2, p.jp, 0)

    def arrive(self, d, after):
        p, h = self.p, self.p.half
        for k, own, u in ((1, True, 1), (0, True, 0), (2, False, 0)):
            j = p.j if own else p.jp
            if d < h:
                for plus in (True, False):
                    slot = 2 * d - 1 if plus else 2 * d
                    self.got(self.unit(slot, j, u), self.zr.at[slot, k])
                    self.ring(slot, plus, d, k, j, u)
                slots = (2 * d - 1, 2 * d)
            else:
                slot = 2 * h - 1
                for part in (0, 1):
                    self.got(self.cut(self.unit(slot, j, u), part), self.zr.at[slot + part, k])
                slots = (slot,)
            for slot in slots:
                if k == 1:
                    self.send(self.unit(slot, j, 1), self.xs.at[slot], self.xr.at[slot], p.partner)
                self.across(slot, k, j, u)
            after(k)

    def arrive_partner(self, slots):
        for slot in slots:
            self.got(self.unit(slot, self.p.jp, 1), self.xr.at[slot])
            self.across(slot, 3, self.p.jp, 1)

    def arrive_sibling(self, slots):
        p = self.p
        for slot in slots:
            for k, (j, u) in enumerate(((p.jc, 0), (p.jc, 1), (p.jcp, 0), (p.jcp, 1))):
                self.got(self.unit(slot, j, u), self.dr.at[slot, k])

    def finish(self):
        for cp in self.sent:
            cp.wait_send()


class KvGather:
    def __init__(self, place, kv, sems):
        self.p, self.kv = place, kv
        self.zs, self.zr, self.xs, self.xr, self.ds, self.dr = sems
        self.sent = []

    def send(self, ref, ss, rs, device):
        cp = remote(ref, ref, ss, rs, device)
        cp.start()
        self.sent.append(cp)

    def got(self, ref, rs):
        remote(ref, ref, self.zs.at[0, 0], rs, self.p.up).wait_recv()

    def ring(self, src_slot, plus, d, k):
        p, h = self.p, self.p.half
        sem = 2 * (d + 1) - 1 if plus else 2 * (d + 1)
        src, dst = self.kv.at[src_slot, p.j], self.kv.at[min(sem, 2 * h - 1), p.j]
        if d + 1 == h:
            part = 0 if plus else 1
            src, dst = src.at[part], dst.at[part]
        device = ((p.up, p.up_other) if plus else (p.down, p.down_other))[k]
        cp = remote(src, dst, self.zs.at[sem, k], self.zr.at[sem, k], device)
        cp.start()
        self.sent.append(cp)

    def across(self, slot, k, j):
        self.send(self.kv.at[slot, j], self.ds.at[slot, k], self.dr.at[slot, k], self.p.sibling)

    def start(self):
        p = self.p
        for k in (0, 1):
            self.ring(0, True, 0, k)
            self.ring(0, False, 0, k)
        self.send(self.kv.at[0, p.j], self.xs.at[0], self.xr.at[0], p.partner)
        self.across(0, 0, p.j)

    def arrive(self, d):
        p, h = self.p, self.p.half
        for slot in slots_of(d, h):
            if d < h:
                self.got(self.kv.at[slot, p.j], self.zr.at[slot, 0])
                for k in (0, 1):
                    self.ring(slot, slot % 2 == 1, d, k)
            else:
                for part in (0, 1):
                    self.got(self.kv.at[slot, p.j, part], self.zr.at[slot + part, 0])
            self.across(slot, 0, p.j)

    def arrive_other(self, d):
        p, h = self.p, self.p.half
        for slot in slots_of(d, h):
            if d == 0:
                self.got(self.kv.at[slot, p.jp], self.xr.at[0])
            elif d < h:
                self.got(self.kv.at[slot, p.jp], self.zr.at[slot, 1])
            else:
                for part in (0, 1):
                    self.got(self.kv.at[slot, p.jp, part], self.zr.at[slot + part, 1])
            self.across(slot, 1, p.jp)

    def arrive_sibling(self, slots):
        p = self.p
        for slot in slots:
            for k, j in enumerate((p.jc, p.jcp)):
                self.got(self.kv.at[slot, j], self.dr.at[slot, k])

    def finish(self):
        for cp in self.sent:
            cp.wait_send()


def slots_of(d, half):
    if d == 0:
        return (0,)
    return (2 * d - 1, 2 * d) if d < half else (2 * half - 1,)


def kernel(
    depth,
    q_hbm, k_hbm, v_hbm, res_hbm, gain_hbm, routes_hbm, gates_hbm, wg_hbm, wu_hbm, wd_hbm,
    attn_out, mix_out,
    q_in, res_in, gain_in, routes_in, gates_in, wg, wu, wd,
    kvg, qs, m_s, l_s, acc_s, att, ss_buf, outgoing, rx, xg, hb, yb, dr_buf, zr_buf, xr_buf, fb, rb, ret, mixed, placed, roots,
    load_sem, g_zs, g_xs, g_ds, a_zr, a_xr, a_dr, b_zr, b_xr, b_dr,
    i_zs, i_zr, i_xs, i_xr, i_ds, i_dr, ss_s, ss_r, x_s, x_r, c_zs, c_zr, c_xs, c_xr, c_ds, c_dr, r_s, r_r,
):
    p = Place(depth)
    half = p.half
    n_exp = EXPERTS

    def load(src, dst, i):
        cp = pltpu.make_async_copy(src, dst, load_sem.at[i])
        cp.start()
        return cp

    loads = [
        load(k_hbm, kvg.at[0, p.j, 0], 0), load(v_hbm, kvg.at[0, p.j, 1], 1), load(q_hbm, q_in, 2),
        load(res_hbm, res_in, 3), load(gain_hbm, gain_in, 4), load(routes_hbm, routes_in, 5),
        load(gates_hbm, gates_in, 6),
    ]

    barrier = pltpu.get_barrier_semaphore()

    def greet(device):
        pl.semaphore_signal(barrier, inc=1, device_id=device, device_id_type=MESH)

    for device in (p.up, p.down, p.up_other, p.down_other, p.partner, p.sibling):
        greet(device)
    for i in range(1, n_exp):
        greet(p.at(p.z, p.j, lax.rem(p.exp + i, n_exp)))
    home = p.exp // 2
    mine = home == p.j
    for i in range(n_exp):
        f = lax.rem(p.exp + i, n_exp)
        if i == 0:
            @pl.when(jnp.logical_not(mine))
            def _():
                greet(p.at(p.z, home, f))
        else:
            greet(p.at(p.z, home, f))
    for u in range(2):
        for jj in range(PLANE):
            src_e = 2 * p.j + u

            @pl.when(jnp.logical_not(jnp.logical_and(jj == p.j, src_e == p.exp)))
            def _():
                greet(p.at(p.z, jj, src_e))
    pl.semaphore_wait(barrier, 6 + (n_exp - 1) + 16 - 2 * mine.astype(jnp.int32))

    loads[0].wait()
    loads[1].wait()

    kv = KvGather(p, kvg, (g_zs, a_zr, g_xs, a_xr, g_ds, a_dr))
    kv.start()

    weight_loads = [load(wg_hbm, wg, 7), load(wu_hbm, wu, 8), load(wd_hbm, wd, 9)]
    for cp in loads[2:]:
        cp.wait()

    for h in range(GROUP):
        qs[pl.ds(h * TOK, TOK), :] = q_in[:, h * HEAD_WIDTH:(h + 1) * HEAD_WIDTH]

    r_row = [routes_in[k:k + 1, :] for k in range(2)]
    expert_ids = lax.broadcasted_iota(jnp.int32, (EXPERTS, TOK), 0)
    one_hot = [(expert_ids == r_row[k]).astype(F32) for k in range(2)]
    earlier = (
        lax.broadcasted_iota(jnp.int32, (TOK, TOK), 0) < lax.broadcasted_iota(jnp.int32, (TOK, TOK), 1)
    ).astype(BF16)
    before = jnp.dot((one_hot[0] + one_hot[1]).astype(BF16), earlier, preferred_element_type=F32)
    slot_row = [jnp.sum(one_hot[k] * before, axis=0, keepdims=True) for k in range(2)]
    dest = [r_row[k] * PITCH + slot_row[k].astype(jnp.int32) for k in range(2)]
    slot_ids = lax.broadcasted_iota(jnp.int32, (EXPERTS * PITCH, TOK), 0)
    match = [slot_ids == dest[k] for k in range(2)]
    dispatch = jnp.where(jnp.logical_or(match[0], match[1]), 1.0, 0.0).astype(F32)
    placed[...] = dispatch
    mixed[...] = jnp.where(match[0], gates_in[0:1, :], 0.0) + jnp.where(match[1], gates_in[1:2, :], 0.0)

    scale = 1.0 / math.sqrt(HEAD_WIDTH)
    kv_rows = PLANE * TOK

    def attend(slot, first):
        keys = kvg[slot, :, 0].reshape(kv_rows, HEAD_WIDTH)
        vals = kvg[slot, :, 1].reshape(kv_rows, HEAD_WIDTH)
        scores = lax.dot_general(qs[...], keys, (((1,), (1,)), ((), ())), preferred_element_type=F32) * scale
        if first:
            at = lax.broadcasted_iota(jnp.int32, scores.shape, 0)
            for h in range(1, GROUP):
                at = at - jnp.where(lax.broadcasted_iota(jnp.int32, scores.shape, 0) >= h * TOK, TOK, 0)
            seen = lax.broadcasted_iota(jnp.int32, scores.shape, 1) <= at + p.j * TOK
            scores = jnp.where(seen, scores, -1e30)
            top = jnp.max(scores, axis=1, keepdims=True)
            terms = jnp.where(seen, jnp.exp(scores - top), 0.0)
            m_s[...] = top
            l_s[...] = jnp.sum(terms, axis=1, keepdims=True)
            acc_s[...] = jnp.dot(terms.astype(BF16), vals, preferred_element_type=F32)
        else:
            old = m_s[...]
            top = jnp.maximum(old, jnp.max(scores, axis=1, keepdims=True))
            fade = jnp.exp(old - top)
            terms = jnp.exp(scores - top)
            m_s[...] = top
            l_s[...] = l_s[...] * fade + jnp.sum(terms, axis=1, keepdims=True)
            acc_s[...] = acc_s[...] * fade + jnp.dot(terms.astype(BF16), vals, preferred_element_type=F32)

    def attend_all(d):
        for slot in slots_of(d, half):
            if slot == 0:
                attend(0, True)
            else:
                if d == half:
                    seen = p.z >= half
                elif slot % 2 == 1:
                    seen = p.z >= d
                else:
                    seen = p.z + d >= depth

                @pl.when(seen)
                def _(slot=slot):
                    attend(slot, False)

    for d in range(1, half + 1):
        kv.arrive(d)
        kv.arrive_other(d - 1)
        kv.arrive_sibling(slots_of(d - 1, half))
        attend_all(d - 1)
    kv.arrive_other(half)
    kv.arrive_sibling(slots_of(half, half))
    attend_all(half)

    for h in range(GROUP):
        rows, cols = slice(h * TOK, (h + 1) * TOK), slice(h * HEAD_WIDTH, (h + 1) * HEAD_WIDTH)
        attn = acc_s[rows, :] / l_s[rows, :]
        attn_out[:, cols] = attn
        att[:, cols] = (res_in[:, cols].astype(F32) + attn).astype(BF16)

    stream = att[...].astype(F32)
    squares = lax.dot_general(
        jnp.ones((8, WIDE), F32), stream * stream, (((1,), (1,)), ((), ())),
        precision=lax.Precision.HIGHEST, preferred_element_type=F32,
    )
    ss_buf[p.exp, :, pl.ds(0, TOK)] = squares
    ss_sends = []
    for i in range(1, n_exp):
        other = lax.rem(p.exp + i, n_exp)
        cp = remote(ss_buf.at[p.exp], ss_buf.at[p.exp], ss_s.at[i], ss_r.at[i], p.at(p.z, p.j, other))
        cp.start()
        ss_sends.append(cp)
    rows_out = jnp.dot(dispatch.astype(BF16), att[...], preferred_element_type=F32)
    outgoing[...] = (rows_out * gain_in[...]).astype(BF16).reshape(EXPERTS, PITCH, WIDE)

    u_me = lax.rem(p.exp, 2)
    x_sends = []
    for i in range(n_exp):
        f = lax.rem(p.exp + i, n_exp)
        cp = remote(outgoing.at[f], rx.at[u_me, p.j], x_s.at[i], x_r.at[u_me, p.j], p.at(p.z, home, f))
        x_sends.append(cp)
        if i == 0:
            pl.when(jnp.logical_not(mine))(cp.start)

            @pl.when(mine)
            def _():
                rx[u_me, p.j] = outgoing[p.exp]
        else:
            cp.start()

    kv.finish()

    for i in range(1, n_exp):
        other = lax.rem(p.exp + n_exp - i, n_exp)
        remote(ss_buf.at[other], ss_buf.at[other], ss_s.at[i], ss_r.at[i], p.up).wait_recv()
    total = ss_buf[0, :, pl.ds(0, TOK)]
    for i in range(1, n_exp):
        total = total + ss_buf[i, :, pl.ds(0, TOK)]
    inverse = lax.rsqrt(total / D + 1e-05)

    own_rows = placed[pl.ds(pl.multiple_of(p.exp * PITCH, PITCH), PITCH), :]
    roots[0, p.j] = jnp.zeros((2, 8, 128), F32)
    inverse_of = lax.dot_general(
        inverse, own_rows, (((1,), (1,)), ((), ())), precision=lax.Precision.HIGHEST, preferred_element_type=F32
    )
    for part in range(2):
        roots[0, p.j, part, :, pl.ds(0, PITCH)] = inverse_of
    iv = KvGather(p, roots, (i_zs, i_zr, i_xs, i_xr, i_ds, i_dr))
    iv.start()

    iv.arrive(1)

    row_ids = lax.broadcasted_iota(jnp.int32, (ROWS, PLANE * PITCH), 0)
    for i in range(1, PLANE):
        row_ids = row_ids + jnp.where(
            lax.broadcasted_iota(jnp.int32, (ROWS, PLANE * PITCH), 0) >= i * CAP, PITCH - CAP, 0
        )
    pack = (row_ids == lax.broadcasted_iota(jnp.int32, (ROWS, PLANE * PITCH), 1)).astype(BF16)

    def columns_of(j, u):
        return pl.ds(pl.multiple_of(j * (2 * WIDE) + u * WIDE, WIDE), WIDE)

    def row_unit(slot, j, u):
        return xg.at[slot, :, columns_of(j, u)]

    def row_half(ref, part):
        return ref.at[pl.ds(part * 80, 80 if part == 0 else ROWS - 80)]

    ag = Gather(p, row_unit, row_half, (g_zs, b_zr, g_xs, b_xr, g_ds, b_dr))
    for u in (1, 0):
        for jj in range(PLANE):
            here = jnp.logical_and(jj == p.j, 2 * p.j + u == p.exp)

            @pl.when(jnp.logical_not(here))
            def _(u=u, jj=jj):
                remote(rx.at[u, jj], rx.at[u, jj], x_s.at[0], x_r.at[u, jj], p.up).wait_recv()

        packed = jnp.dot(pack, rx[u].reshape(PLANE * PITCH, WIDE), preferred_element_type=F32)
        xg[0, :, columns_of(p.j, u)] = packed.astype(BF16)
        ag.start(u)
    for cp in weight_loads:
        cp.wait()
    ag.start_partner()
    iv.arrive(2)

    lane_ids = lax.broadcasted_iota(jnp.int32, (ROWS, 128), 1)
    line_ids = lax.broadcasted_iota(jnp.int32, (ROWS, 128), 0)

    def roots_of(slot):
        spread = jnp.zeros((ROWS, 128), F32)
        for jj in range(PLANE):
            at = jnp.logical_and(line_ids - jj * CAP == lane_ids, lane_ids < CAP)
            spread = spread + jnp.where(at, roots[slot, jj, 0, 0:1, :], 0.0)
        return jnp.sum(spread, axis=1, keepdims=True)

    def hidden(lo, hi):
        count = hi - lo
        root = jnp.concatenate([roots_of(slot) for slot in range(lo, hi)], axis=0)
        rows = xg[lo:hi].reshape(count * ROWS, D)
        gate = lax.dot_general(rows, wg[...], (((1,), (1,)), ((), ())), preferred_element_type=F32)
        up = lax.dot_general(rows, wu[...], (((1,), (1,)), ((), ())), preferred_element_type=F32)
        gate, up = gate * root, up * root
        act = gate / (1.0 + jnp.exp(-gate)) * up
        hb[lo:hi] = act.astype(BF16).reshape(count, ROWS, FF_LOCAL)

    def hidden_all(d):
        slots = slots_of(d, half)
        iv.arrive_other(d)
        iv.arrive_sibling(slots)
        hidden(slots[0], slots[-1] + 1)

    sent = []

    def send(src, dst, ss, rs, device):
        cp = remote(src, dst, ss, rs, device)
        cp.start()
        sent.append(cp)

    def wait_for(ref, rs):
        remote(ref, ref, c_zs.at[0, 0], rs, p.up).wait_recv()

    def wide_columns(j):
        return pl.ds(pl.multiple_of(j * (2 * WIDE), 2 * WIDE), 2 * WIDE)

    def produce(slot):
        def part(n, _):
            cols = pl.ds(pl.multiple_of(n * WIDE, WIDE), WIDE)
            yb[slot, :, cols] = jnp.dot(hb[slot], wd[:, cols], preferred_element_type=F32).astype(BF16)
            return 0

        lax.fori_loop(0, D // WIDE, part, 0)
        for k, j in enumerate((p.jc, p.jcp)):
            send(yb.at[slot, :, wide_columns(j)], dr_buf.at[slot, k], c_ds.at[slot, k], c_dr.at[slot, k], p.sibling)

    def for_partner(slot):
        for k in range(2):
            wait_for(dr_buf.at[slot, k], c_dr.at[slot, k])
        cols = columns_of(p.jp, 1)
        yb[slot, :, cols] = (yb[slot, :, cols].astype(F32) + dr_buf[slot, 1, :, WIDE:].astype(F32)).astype(BF16)
        send(yb.at[slot, :, cols], xr_buf.at[slot], c_xs.at[slot], c_xr.at[slot], p.partner)

    def halves(ref, part):
        return ref.at[:, pl.ds(part * (WIDE // 2), WIDE // 2)]

    def reduce_unit(slot, d, k):
        for j, u in (((p.j, 0), (p.j, 1), (p.jp, 0))[k],):
            cols = columns_of(j, u)
            own = k != 2
            total = yb[slot, :, cols].astype(F32)
            total = total + dr_buf[slot, 0 if own else 1, :, pl.ds(u * WIDE, WIDE)].astype(F32)
            if k == 1:
                wait_for(xr_buf.at[slot], c_xr.at[slot])
                total = total + xr_buf[slot].astype(F32)
            if d == half:
                yb[slot, :, cols] = total.astype(BF16)
            elif d == half - 1:
                part = 0 if slot % 2 == 1 else 1
                wait_for(halves(zr_buf.at[slot, k], part), c_zr.at[slot, k])
                cut = slice(part * (WIDE // 2), (part + 1) * (WIDE // 2))
                keep = slice((1 - part) * (WIDE // 2), (2 - part) * (WIDE // 2))
                zr = zr_buf[slot, k, :, cut].astype(F32)
                base = j * (2 * WIDE) + u * WIDE
                for piece, value in ((cut, total[:, cut] + zr), (keep, total[:, keep])):
                    at = pl.ds(pl.multiple_of(base + piece.start, WIDE // 2), WIDE // 2)
                    yb[slot, :, at] = value.astype(BF16)
            else:
                sources = (0, 2 * half - 1) if slot == 0 else (slot,)
                for i in sources:
                    wait_for(zr_buf.at[i, k], c_zr.at[i, k])
                    total = total + zr_buf[i, k].astype(F32)
                yb[slot, :, cols] = total.astype(BF16)
            if d == 0:
                if k == 2:
                    send(yb.at[slot, :, cols], xr_buf.at[8], c_xs.at[8], c_xr.at[8], p.partner)
            elif d == half:
                for part in (0, 1):
                    to = 2 * (d - 1) - 1 + part
                    base = j * (2 * WIDE) + u * WIDE + part * (WIDE // 2)
                    send(
                        yb.at[slot, :, pl.ds(pl.multiple_of(base, WIDE // 2), WIDE // 2)],
                        halves(zr_buf.at[to, k], part),
                        c_zs.at[slot + part, k], c_zr.at[to, k], p.down if part == 0 else p.up,
                    )
            else:
                plus = slot % 2 == 1
                if d == 1:
                    to = 0 if plus else 2 * half - 1
                else:
                    to = slot - 2
                send(
                    yb.at[slot, :, cols], zr_buf.at[to, k], c_zs.at[slot, k], c_zr.at[to, k],
                    p.down if plus else p.up,
                )

    last, next_in = slots_of(half, half), slots_of(half - 1, half)
    for d in range(1, half + 1):
        near = slots_of(d - 1, half)

        def between(k):
            if k == 1:
                ag.arrive_partner(near)
            elif k == 0:
                ag.arrive_sibling(near)
                hidden_all(d - 1)
            elif d + 2 <= half:
                iv.arrive(d + 2)

        ag.arrive(d, between)
    ag.arrive_partner(last)
    produce(next_in[0])
    ag.arrive_sibling(last)

    hidden_all(half)
    for s in last:
        produce(s)
    for_partner(next_in[0])
    for s in next_in[1:]:
        produce(s)
    for s in last:
        for_partner(s)
    for d in range(half, 0, -1):
        for k in (2, 0):
            for s in slots_of(d, half):
                reduce_unit(s, d, k)
        for s in slots_of(d - 1, half):
            if s != next_in[0]:
                for_partner(s)
        if d < half:
            for s in slots_of(d + 1, half):
                reduce_unit(s, d + 1, 1)
        if d > 1:
            for s in slots_of(d - 2, half):
                produce(s)

    r_sends = []

    def give_back(u):
        spread = lax.dot_general(pack, fb[u], (((0,), (0,)), ((), ())), preferred_element_type=F32)
        rb[u] = spread.astype(BF16).reshape(PLANE, PITCH, WIDE)
        for jj in range(PLANE):
            here = jnp.logical_and(jj == p.j, 2 * p.j + u == p.exp)
            cp = remote(rb.at[u, jj], ret.at[p.exp], r_s.at[u * PLANE + jj], r_r.at[p.exp], p.at(p.z, jj, 2 * p.j + u))
            r_sends.append((here, cp))
            pl.when(jnp.logical_not(here))(cp.start)

            @pl.when(here)
            def _():
                ret[p.exp] = rb[u, jj]

    reduce_unit(0, 0, 2)
    reduce_unit(0, 0, 0)
    for s in slots_of(1, half):
        reduce_unit(s, 1, 1)
    wait_for(xr_buf.at[8], c_xr.at[8])
    fb[0] = (yb[0, :, columns_of(p.j, 0)].astype(F32) + xr_buf[8].astype(F32)).astype(BF16)
    give_back(0)
    reduce_unit(0, 0, 1)
    fb[1] = yb[0, :, columns_of(p.j, 1)]
    give_back(1)

    ag.finish()
    iv.finish()
    for cp in sent:
        cp.wait_send()
    for cp in ss_sends:
        cp.wait_send()
    for i, cp in enumerate(x_sends):
        if i == 0:
            pl.when(jnp.logical_not(mine))(cp.wait_send)
        else:
            cp.wait_send()

    for i in range(n_exp):
        f = lax.rem(p.exp + i, n_exp)
        cp = remote(ret.at[f], ret.at[f], r_s.at[0], r_r.at[f], p.up)
        if i == 0:
            pl.when(jnp.logical_not(mine))(cp.wait_recv)
        else:
            cp.wait_recv()
    returned = ret[...].reshape(EXPERTS * PITCH, WIDE).astype(F32)
    mix_out[...] = lax.dot_general(
        mixed[...], returned, (((0,), (0,)), ((), ())), precision=lax.Precision.HIGHEST, preferred_element_type=F32
    )
    for here, cp in r_sends:
        pl.when(jnp.logical_not(here))(cp.wait_send)


def shards(depth, queries, keys, values, residual, norm_gain, routes, gates, w_gate, w_up, w_down):
    hbm_spec = pl.BlockSpec(memory_space=pltpu.HBM)
    vmem_spec = pl.BlockSpec(memory_space=pltpu.VMEM)
    slots = depth
    vmem, dma = pltpu.VMEM, pltpu.SemaphoreType.DMA
    tok_block = jax.ShapeDtypeStruct((TOK, WIDE), F32)
    scratch = [
        vmem((TOK, WIDE), BF16), vmem((TOK, WIDE), BF16), vmem((1, WIDE), F32), vmem((2, TOK), jnp.int32),
        vmem((2, TOK), F32), vmem((FF_LOCAL, D), BF16), vmem((FF_LOCAL, D), BF16), vmem((FF_LOCAL, D), BF16),
        vmem((slots, PLANE, 2, TOK, HEAD_WIDTH), BF16),
        vmem((GROUP * TOK, HEAD_WIDTH), BF16), vmem((GROUP * TOK, 1), F32), vmem((GROUP * TOK, 1), F32),
        vmem((GROUP * TOK, HEAD_WIDTH), F32), vmem((TOK, WIDE), BF16), vmem((EXPERTS, 8, 128), F32),
        vmem((EXPERTS, PITCH, WIDE), BF16), vmem((2, PLANE, PITCH, WIDE), BF16),
        vmem((slots, ROWS, D), BF16), vmem((slots, ROWS, FF_LOCAL), BF16), vmem((slots, ROWS, D), BF16),
        vmem((slots, 2, ROWS, 2 * WIDE), BF16), vmem((slots, 3, ROWS, WIDE), BF16), vmem((9, ROWS, WIDE), BF16),
        vmem((2, ROWS, WIDE), BF16), vmem((2, PLANE, PITCH, WIDE), BF16), vmem((EXPERTS, PITCH, WIDE), BF16),
        vmem((EXPERTS * PITCH, TOK), F32), vmem((EXPERTS * PITCH, TOK), F32), vmem((slots, PLANE, 2, 8, 128), F32),
        dma((10,)),
        dma((9, 3)), dma((9,)), dma((8, 4)),
        dma((9, 2)), dma((1,)), dma((8, 2)),
        dma((9, 3)), dma((9,)), dma((8, 4)),
        dma((9, 2)), dma((9, 2)), dma((1,)), dma((1,)), dma((8, 2)), dma((8, 2)),
        dma((8,)), dma((8,)), dma((8,)), dma((2, PLANE)),
        dma((9, 3)), dma((9, 3)), dma((9,)), dma((9,)), dma((8, 2)), dma((8, 2)),
        dma((8,)), dma((8,)),
    ]
    attn, mix = pl.pallas_call(
        functools.partial(kernel, depth),
        out_shape=(tok_block, tok_block),
        in_specs=[hbm_spec] * 10,
        out_specs=(vmem_spec, vmem_spec),
        scratch_shapes=scratch,
        compiler_params=pltpu.CompilerParams(
            collective_id=0, has_side_effects=True, vmem_limit_bytes=VMEM_BYTES
        ),
    )(
        queries, keys, values, residual, norm_gain.reshape(1, WIDE), routes.T, gates.T,
        w_gate[0].T, w_up[0].T, w_down[0],
    )
    attended = lax.reduce_precision(residual.astype(F32) + attn, 8, 7)
    return attended.astype(BF16), (attended + mix).astype(BF16)


def solution(mesh):
    in_specs = (
        P("seq", "exp"), P("seq", "exp"), P("seq", "exp"), P("seq", "exp"), P("exp"), P("seq", None), P("seq", None),
        P("exp", None, "seq"), P("exp", None, "seq"), P("exp", "seq", None),
    )
    body = functools.partial(shards, mesh.shape["seq"] // PLANE)
    return jax.shard_map(body, mesh=mesh, in_specs=in_specs, out_specs=(P("seq", "exp"), P("seq", "exp")), check_vma=False)
```
